32 devices in a mesh: ia: 4 (over y, x), ja: 4 (over z), ka: 2 (over core).
Axes of the slice: x: 2, y: 2, z: 4, core: 2. Of those that a mesh axis runs over, the one named last changes fastest.
Arguments:
- tensor: bfloat16 [1024, 512, 256], P('ia', 'ja', 'ka'), may hold values from -6 to 6
- factor_b: bfloat16 [512, 256], P('ja', 'ka'), may hold values from -16 to 16
- factor_c: bfloat16 [256, 256], P('ka', 'ja'), may hold values from -16 to 16
Outputs:
- factor_a: float32 [1024, 256], P(('ia', 'ja', 'ka'))
The draws below stay inside these ranges and needn't reach their ends.
All inputs are finite; a program needn't handle non-finite values.
Results may differ from the reference program's by a relative error of at most 0.0003.
Values may be sent and summed in bfloat16 or wider, within the bound.
No kernel may reach another device: no remote copies, remote signals or barrier semaphores. Data moves between devices by JAX's collectives and lax.ppermute only.
A program may use at most 64 MiB of HBM per device.

```python
import jax
import jax.numpy as jnp
from jax import lax

R = 256
I = 1024
J = 512
K = 256


def draw_factor(key, length):
    k_place, k_shared, k_noise = jax.random.split(key, 3)
    common = 1.0
    place = (jnp.arange(length, dtype=jnp.float32) + jax.random.uniform(k_place, (length,), jnp.float32)) / length
    scales = 10.0 ** place
    shared = jnp.clip(jax.random.normal(k_shared, (length, 1), jnp.float32), -6.0, 6.0)
    noise = jnp.clip(jax.random.normal(k_noise, (length, R), jnp.float32), -6.0, 6.0)
    raw = scales[:, None] * (shared + noise)
    total = jnp.sum(scales * scales) * (common + 1.0)
    return (raw / jnp.sqrt(total)).astype(jnp.bfloat16)


def draw_factor_b(key, part):
    return draw_factor(jax.random.fold_in(key, 11), J)


def draw_factor_c(key, part):
    return draw_factor(jax.random.fold_in(key, 23), K)


def shard_levels(stream_key, extent, cuts, least, largest):
    def one(dim, blocks):
        steps = jax.random.uniform(jax.random.fold_in(jax.random.fold_in(stream_key, 6), dim), (blocks,), jnp.float32, least / len(cuts), largest / len(cuts))
        return jnp.repeat(jnp.exp(steps), extent[dim] // blocks).reshape((-1,) + (1,) * (len(extent) - dim - 1))

    level = one(*cuts[0])
    for cut in cuts[1:]:
        level = level * one(*cut)
    return level


def normal_values(own_key, dims, scale, limit, cuts=(), held_as=jnp.bfloat16):
    drawn = jax.random.normal(own_key, dims, jnp.float32) * scale
    if len(cuts) > 0:
        drawn = shard_levels(own_key, dims, cuts, -0.22, 0.18) * drawn
    return jnp.clip(drawn, min=-limit, max=limit).astype(held_as)


def setup_inputs(seed: int = 0) -> dict:
    seeds = jax.random.split(jax.random.key(seed), 4)
    return {
        "tensor": normal_values(seeds[0], (I, J, K), 1.0, 6.0, ((0, 4), (1, 4), (2, 2))),
        "factor_b": draw_factor_b(jax.random.fold_in(seeds[3], 71), 0),
        "factor_c": draw_factor_c(jax.random.fold_in(seeds[3], 71), 0),
    }


ridge_weight = 0.1

def contract(block, factor_b, factor_c):
    rows, width_j, width_k = block.shape
    inner = jnp.dot(block.reshape(rows * width_j, width_k).astype(jnp.float32), factor_c.astype(jnp.float32), preferred_element_type=jnp.float32)
    inner = inner.reshape(rows, width_j, -1)
    return jnp.sum(inner * factor_b.astype(jnp.float32)[None], axis=1)

def reference(tensor, factor_b, factor_c):
    gram_b = jnp.dot(factor_b.T.astype(jnp.float32), factor_b.astype(jnp.float32), preferred_element_type=jnp.float32)
    gram_c = jnp.dot(factor_c.T.astype(jnp.float32), factor_c.astype(jnp.float32), preferred_element_type=jnp.float32)
    normal_matrix = gram_b * gram_c + ridge_weight * jnp.eye(R, dtype=jnp.float32)
    blocks = tensor.reshape(I // 16, 16, J, K)
    mttkrp = lax.map(lambda piece: contract(piece, factor_b, factor_c), blocks).reshape(I, R)
    lower = jnp.linalg.cholesky(normal_matrix)
    solved = jax.scipy.linalg.cho_solve((lower, True), mttkrp.T)
    return solved.T
```

```python
import functools

import jax
import jax.numpy as jnp
from jax import lax
from jax.experimental import pallas as pl
from jax.experimental.pallas import tpu as pltpu
from jax.sharding import PartitionSpec as P

ridge_weight = 0.1
exact = lax.Precision.HIGHEST
vmem = pl.BlockSpec(memory_space=pltpu.VMEM)
smem = pl.BlockSpec(memory_space=pltpu.SMEM)
hbm = pl.BlockSpec(memory_space=pl.ANY)


def shift(n, s):
    return [(i, (i + s) % n) for i in range(n)]


def wrap(x, n):
    return lax.rem(x + n, n)


def mttkrp_kernel(nj, nk, height_b, flipped, where, block, *refs):
    c_parts, refs = refs[:nj], refs[nj:]
    b_parts, refs = refs[:nk], refs[nk:]
    out, held, c_rows, b_rows, arrived = refs
    me_j, me_k = where[0], where[1]
    owned = out.shape[2]

    def owner_rows(turn):
        t, u = nk - 1 - turn // nj, turn % nj
        to = wrap(me_j + u, nj) * nk + wrap(me_k + t, nk)
        return t, u, pl.multiple_of(to * owned, owned)

    def load(turn):
        _, _, first = owner_rows(turn)
        rows = pl.ds(first, owned)
        return pltpu.make_async_copy(block.at[rows], held.at[rows], arrived.at[turn])

    for turn in range(nj * nk):
        load(turn).start()
    width_c = c_parts[0].shape[0] - height_b
    for s in range(nj):
        at = pl.multiple_of(wrap(me_j - s, nj) * width_c, width_c)
        c_rows[pl.ds(at, width_c), :] = c_parts[s][height_b:, :]
    for t in range(nk):
        at = pl.multiple_of(wrap(me_k - t, nk) * height_b, height_b)
        if flipped:
            b_rows[pl.ds(at, height_b), :] = b_parts[t][:height_b, :]
        else:
            at = pl.multiple_of(wrap(me_k - t, nk) * 128, 128)
            b_rows[:, pl.ds(at, 128)] = b_parts[t][:height_b, :]
    c_wide = c_rows[...].T
    b_wide = (b_rows[...].T if flipped else b_rows[...]).astype(jnp.float32)

    def step(turn, _):
        load(turn).wait()
        t, u, first = owner_rows(turn)
        sums = []
        for i in range(owned):
            inner = jnp.dot(held[first + i], c_wide, preferred_element_type=jnp.float32)
            sums.append(jnp.sum(inner * b_wide, axis=0, keepdims=True))
        out[t, u] = jnp.concatenate(sums, axis=0)
        return 0

    lax.fori_loop(0, nj * nk, step, 0)


def mttkrp(where, tensor, c_parts, b_parts, height_b, flipped, nj, nk, rank):
    rows, width_j, width_k = tensor.shape
    owned = rows // (nj * nk)
    b_shape = (rank, width_j) if flipped else (width_j, rank)
    return pl.pallas_call(
        functools.partial(mttkrp_kernel, nj, nk, height_b, flipped),
        out_shape=jax.ShapeDtypeStruct((nk, nj, owned, rank), jnp.float32),
        in_specs=[smem, hbm] + [vmem] * (nj + nk),
        out_specs=vmem,
        scratch_shapes=[
            pltpu.VMEM(tensor.shape, tensor.dtype),
            pltpu.VMEM((rank, width_k), tensor.dtype),
            pltpu.VMEM(b_shape, tensor.dtype),
            pltpu.SemaphoreType.DMA((nj * nk,)),
        ],
        compiler_params=pltpu.CompilerParams(vmem_limit_bytes=40 * 2**20),
        cost_estimate=pl.CostEstimate(
            flops=2 * rows * width_j * width_k * rank,
            bytes_accessed=2 * rows * width_j * width_k,
            transcendentals=0,
        ),
    )(where, tensor, *c_parts, *b_parts)


def column(x, q):
    return jnp.broadcast_to(x[:, q : q + 1], x.shape)


def row(x, q):
    return jnp.broadcast_to(x[q : q + 1, :], x.shape)


def invert(a, step=16):
    size = a.shape[0]
    groups, per = size // 8, step // 8
    rows = [a[8 * i : 8 * i + 8, :] for i in range(groups)]
    lane = lax.broadcasted_iota(jnp.int32, (8, size), 1)
    sub = lax.broadcasted_iota(jnp.int32, (8, size), 0)
    for first in range(0, size, step):
        g0 = first // 8
        cols = [[column(r, first + q) for q in range(step)] for r in rows]
        inside = (lane >= first) & (lane < first + step)
        panel = rows[g0 : g0 + per]
        c = [[cols[g0 + i][q] for i in range(per)] for q in range(step)]
        for q in range(step):
            gq, sq = q // 8, q % 8
            here = sub == sq
            inv = 1.0 / row(c[q][gq], sq)
            pivot_row = jnp.where(lane == first + q, inv, row(panel[gq], sq) * inv)
            for i in range(per):
                new = jnp.where(lane == first + q, 0.0, panel[i]) - c[q][i] * pivot_row
                panel[i] = jnp.where(here, pivot_row, new) if i == gq else new
            for p in range(q + 1, step):
                scaled = row(c[p][gq], sq) * inv
                for i in range(per):
                    new = c[p][i] - c[q][i] * scaled
                    c[p][i] = jnp.where(here, scaled, new) if i == gq else new
        spread = [row(panel[q // 8], q % 8) for q in range(step)]
        for i in range(groups):
            if g0 <= i < g0 + per:
                rows[i] = panel[i - g0]
                continue
            update = cols[i][0] * spread[0]
            for q in range(1, step):
                update = update + cols[i][q] * spread[q]
            rows[i] = jnp.where(inside, 0.0, rows[i]) - update
    return jnp.concatenate(rows, axis=0)


def dot_t(x, y):
    return lax.dot_general(
        x, y, (((1,), (1,)), ((), ())), preferred_element_type=jnp.float32, precision=exact
    )


def head_kernel(nj, nk, height_b, flipped, where, *refs):
    parts, refs = refs[: nj * nk], refs[nj * nk :]
    top_out, cross_out, rest_out, b_all, c_all = refs
    me_j, me_k = where[0], where[1]
    half = cross_out.shape[0]
    width_c = parts[0].shape[0] - height_b
    height = b_all.shape[1]
    for s in range(nj):
        for t in range(nk):
            part = parts[s * nk + t]
            at = pl.multiple_of(wrap(me_j - s, nj) * width_c, width_c)
            c_all[t, pl.ds(at, width_c), :] = part[height_b:, :]
            if flipped:
                at = pl.multiple_of(wrap(me_k - t, nk) * height_b, height_b)
                b_all[s, pl.ds(at, height_b), :] = part[:height_b, :]
            else:
                at = pl.multiple_of(wrap(me_k - t, nk) * 128, 128)
                b_all[s, :, pl.ds(at, 128)] = part[:height_b, :]

    def gram(x, contracted):
        dims = (((contracted,), (contracted,)), ((), ()))
        return lax.dot_general(x, x, dims, preferred_element_type=jnp.float32)

    if flipped:
        gram_b = sum(gram(b_all[s], 1) for s in range(nj))
    else:
        gram_b = gram(b_all[...].reshape(nj * height, 2 * half), 0)
    gram_c = sum(gram(c_all[t], 1) for t in range(nk))
    size = 2 * half
    diagonal = lax.broadcasted_iota(jnp.int32, (size, size), 0) == lax.broadcasted_iota(
        jnp.int32, (size, size), 1
    )
    normal = gram_b * gram_c + jnp.where(diagonal, ridge_weight, 0.0)
    top = invert(normal[:half, :half])
    right = normal[:half, half:]
    cross = jnp.dot(top, right, precision=exact, preferred_element_type=jnp.float32)
    top_out[...] = top
    cross_out[...] = cross
    rest_out[...] = normal[half:, half:] - jnp.dot(
        right.T, cross, precision=exact, preferred_element_type=jnp.float32
    )


def tail_kernel(*refs):
    rows, (top, cross, rest, out) = refs[:-4], refs[-4:]
    half = cross.shape[0]
    mine = rows[0][...]
    for r in rows[1:]:
        mine = mine + r[...]
    left, right = mine[:, :half], mine[:, half:]
    dot = functools.partial(jnp.dot, precision=exact, preferred_element_type=jnp.float32)
    reduced = right - dot(left, cross[...])
    partial = dot(left, top[...])
    solved = dot(reduced, invert(rest[...]))
    out[:, half:] = solved
    out[:, :half] = partial - dot_t(solved, cross[...])


def body(tensor, factor_b, factor_c):
    nj, nk = lax.axis_size("ja"), lax.axis_size("ka")
    where = jnp.stack([lax.axis_index("ja"), lax.axis_index("ka")]).astype(jnp.int32)
    rank = factor_b.shape[1] * nk
    half = rank // 2
    flipped = factor_b.shape[1] % 128 != 0
    part_b = factor_b.T if flipped else factor_b
    height_b = part_b.shape[0]
    mine = jnp.concatenate([part_b, factor_c.T], axis=0)
    line = [mine] + [lax.ppermute(mine, "ja", shift(nj, s)) for s in range(1, nj)]
    parts = [[x] + [lax.ppermute(x, "ka", shift(nk, t)) for t in range(1, nk)] for x in line]
    sums = mttkrp(where, tensor, line, parts[0], height_b, flipped, nj, nk, rank)
    total = sums[0]
    for t in range(1, nk):
        total = total + lax.ppermute(sums[t], "ka", shift(nk, t))
    rows = [total[0]] + [lax.ppermute(total[u], "ja", shift(nj, u)) for u in range(1, nj)]
    flat = [x for group in parts for x in group]
    square = jax.ShapeDtypeStruct((half, half), jnp.float32)
    b_shape = (nj, rank, part_b.shape[1]) if flipped else (nj, height_b, rank)
    top, cross, rest = pl.pallas_call(
        functools.partial(head_kernel, nj, nk, height_b, flipped),
        out_shape=[square] * 3,
        in_specs=[smem] + [vmem] * len(flat),
        out_specs=[vmem] * 3,
        scratch_shapes=[
            pltpu.VMEM(b_shape, factor_b.dtype),
            pltpu.VMEM((nk, rank, factor_c.shape[0]), factor_c.dtype),
        ],
        compiler_params=pltpu.CompilerParams(vmem_limit_bytes=40 * 2**20),
        cost_estimate=pl.CostEstimate(flops=10**10, bytes_accessed=2**20, transcendentals=0),
    )(where, *flat)
    return pl.pallas_call(
        tail_kernel,
        out_shape=jax.ShapeDtypeStruct((rows[0].shape[0], rank), jnp.float32),
        in_specs=[vmem] * (len(rows) + 3),
        out_specs=vmem,
        compiler_params=pltpu.CompilerParams(vmem_limit_bytes=40 * 2**20),
        cost_estimate=pl.CostEstimate(flops=10**10, bytes_accessed=2**20, transcendentals=0),
    )(*rows, top, cross, rest)


def solution(mesh):
    placed = (P("ia", "ja", "ka"), P("ja", "ka"), P("ka", "ja"))
    return jax.shard_map(
        body, mesh=mesh, in_specs=placed, out_specs=P(("ia", "ja", "ka"), None), check_vma=False
    )
```

```python
import functools

import jax
import jax.numpy as jnp
from jax import lax
from jax.experimental import pallas as pl
from jax.experimental.pallas import tpu as pltpu
from jax.sharding import PartitionSpec as P

ridge_weight = 0.1
exact = lax.Precision.HIGHEST
vmem = pl.BlockSpec(memory_space=pltpu.VMEM)
smem = pl.BlockSpec(memory_space=pltpu.SMEM)
hbm = pl.BlockSpec(memory_space=pltpu.HBM)


def shift(n, s):
    return [(i, (i + s) % n) for i in range(n)]


def wrap(x, n):
    return lax.rem(x + n, n)


def owner(nj, nk, where, t, u):
    return wrap(where[0] + u, nj) * nk + wrap(where[1] + t, nk)


def fetch_kernel(nj, nk, where, block, held, arrived):
    owned = held.shape[2]
    copies = []
    for t in range(nk):
        for u in range(nj):
            first = pl.multiple_of(owner(nj, nk, where, t, u) * owned, owned)
            copies.append(
                pltpu.make_async_copy(
                    block.at[pl.ds(first, owned)], held.at[t, u], arrived.at[t * nj + u]
                )
            )
    for copy in copies:
        copy.start()
    for copy in copies:
        copy.wait()


def fetch(where, tensor, nj, nk):
    rows, width_j, width_k = tensor.shape
    owned = rows // (nj * nk)
    return pl.pallas_call(
        functools.partial(fetch_kernel, nj, nk),
        out_shape=jax.ShapeDtypeStruct((nk, nj, owned, width_j, width_k), tensor.dtype),
        in_specs=[smem, hbm],
        out_specs=vmem,
        scratch_shapes=[pltpu.SemaphoreType.DMA((nj * nk,))],
        compiler_params=pltpu.CompilerParams(vmem_limit_bytes=20 * 2**20),
        cost_estimate=pl.CostEstimate(
            flops=4 * 10**9, bytes_accessed=2 * rows * width_j * width_k, transcendentals=0
        ),
    )(where, tensor)


def contract(held, t, out, c_wide, b_wide):
    nj, owned = held.shape[1], held.shape[2]

    def step(u, _):
        sums = []
        for i in range(owned):
            inner = jnp.dot(held[t, u, i], c_wide, preferred_element_type=jnp.float32)
            sums.append(jnp.sum(inner * b_wide, axis=0, keepdims=True))
        out[u] = jnp.concatenate(sums, axis=0)
        return 0

    lax.fori_loop(0, nj, step, 0)


def away_kernel(nj, nk, height_b, flipped, where, held, *refs):
    line, refs = refs[:nj], refs[nj:]
    b_parts, refs = refs[:nk], refs[nk:]
    out, c_out, b_out, c_cols, b_cols, b_rows = refs
    width_c = line[0].shape[0] - height_b
    for s in range(nj):
        at = pl.multiple_of(wrap(where[0] - s, nj) * width_c, width_c)
        c_out[pl.ds(at, width_c), :] = line[s][height_b:, :]
        b_out[s] = line[s][:height_b, :]
    for t in range(nk):
        if flipped:
            at = pl.multiple_of(wrap(where[1] - t, nk) * height_b, height_b)
            b_rows[pl.ds(at, height_b), :] = b_parts[t][:height_b, :]
        else:
            at = pl.multiple_of(wrap(where[1] - t, nk) * 128, 128)
            b_rows[:, pl.ds(at, 128)] = b_parts[t][:height_b, :]
    c_cols[...] = c_out[...].T
    b_cols[...] = (b_rows[...].T if flipped else b_rows[...]).astype(jnp.float32)
    for t in range(1, nk):
        contract(held, t, out.at[t - 1], c_cols[...], b_cols[...])


def home_kernel(held, c_cols, b_cols, out):
    contract(held, 0, out, c_cols[...], b_cols[...])


def mttkrp(where, held, line, b_parts, height_b, flipped, rank):
    nk, nj, owned, width_j, width_k = held.shape
    flops = 2 * nj * owned * width_j * width_k * rank
    params = pltpu.CompilerParams(vmem_limit_bytes=20 * 2**20)

    def cost(count):
        return pl.CostEstimate(flops=count * flops, bytes_accessed=2**20, transcendentals=0)

    away, c_own, b_own, c_cols, b_cols = pl.pallas_call(
        functools.partial(away_kernel, nj, nk, height_b, flipped),
        out_shape=[
            jax.ShapeDtypeStruct((nk - 1, nj, owned, rank), jnp.float32),
            jax.ShapeDtypeStruct((rank, width_k), held.dtype),
            jax.ShapeDtypeStruct((nj, height_b, line[0].shape[1]), held.dtype),
            jax.ShapeDtypeStruct((width_k, rank), held.dtype),
            jax.ShapeDtypeStruct((width_j, rank), jnp.float32),
        ],
        in_specs=[smem] + [vmem] * (1 + nj + nk),
        out_specs=[vmem] * 5,
        scratch_shapes=[pltpu.VMEM((rank, width_j) if flipped else (width_j, rank), held.dtype)],
        compiler_params=params,
        cost_estimate=cost(nk - 1),
    )(where, held, *line, *b_parts)
    home = pl.pallas_call(
        home_kernel,
        out_shape=jax.ShapeDtypeStruct((nj, owned, rank), jnp.float32),
        in_specs=[vmem] * 3,
        out_specs=vmem,
        compiler_params=params,
        cost_estimate=cost(1),
    )(held, c_cols, b_cols)
    return home, away, c_own, b_own


def column(x, q):
    return jnp.broadcast_to(x[:, q : q + 1], x.shape)


def row(x, q):
    return jnp.broadcast_to(x[q : q + 1, :], x.shape)


def thirds(x):
    high = x.astype(jnp.bfloat16)
    x = x - high.astype(jnp.float32)
    middle = x.astype(jnp.bfloat16)
    return high, middle, (x - middle.astype(jnp.float32)).astype(jnp.bfloat16)


def stack(tiles):
    return jnp.concatenate([jnp.concatenate(r, axis=1) for r in tiles], axis=0)


def invert(a, step=16):
    size = a.shape[0]
    wide, per = size // 128, step // 8
    lane = lax.broadcasted_iota(jnp.int32, (8, 128), 1)
    sub = lax.broadcasted_iota(jnp.int32, (8, 128), 0)

    def tile(g, w):
        return a[8 * g : 8 * g + 8, 128 * w : 128 * w + 128]

    def columns(rows, w, first):
        return [[column(r[w], first + q) for r in rows] for q in range(step)]

    now = [[tile(g, w) for w in range(wide)] for g in range(per)]
    for first in range(0, size, step):
        g0, w0, lane0 = first // 8, first // 128, first % 128
        inside = (lane >= lane0) & (lane < lane0 + step)
        more = first + step < size
        panel = [list(r) for r in now]
        c = columns(now, w0, lane0)
        if more:
            ahead = [[tile(g0 + per + i, w) for w in range(wide)] for i in range(per)]
            ahead_c = columns(ahead, w0, lane0)
        scale = [jnp.zeros((8, 128), jnp.float32)] * per
        pivot = row(c[0][0], 0)
        for q in range(step):
            gq, sq = q // 8, q % 8
            here = sub == sq
            inv = 1.0 / pivot
            scale[gq] = jnp.where(here, inv, scale[gq])
            if q + 1 < step:
                gn, sn = (q + 1) // 8, (q + 1) % 8
                product = row(c[q][gn], sn) * row(c[q + 1][gq], sq)
                pivot = row(c[q + 1][gn], sn) - product * inv
            factor = [jnp.where(here, 0.0, c[q][i]) if i == gq else c[q][i] for i in range(per)]
            for i in range(per):
                unit = jnp.where(here, 1.0, 0.0) if i == gq else 0.0
                panel[i][w0] = jnp.where(lane == lane0 + q, unit, panel[i][w0])
            for w in range(wide):
                scaled = row(panel[gq][w], sq) * inv
                for i in range(per):
                    panel[i][w] = panel[i][w] - factor[i] * scaled
            for p in range(q + 1, step):
                scaled = row(c[p][gq], sq) * inv
                for i in range(per):
                    c[p][i] = c[p][i] - factor[i] * scaled
        done = [[panel[i][w] * scale[i] for w in range(wide)] for i in range(per)]
        lanes = lax.broadcasted_iota(jnp.int32, (step, size), 1)
        left = stack(now)
        left = thirds(jnp.where(lanes < first, -left, left))
        right = thirds(stack(done))
        pairs = ((0, 0), (0, 1), (1, 0), (0, 2), (1, 1), (2, 0))
        update = lax.dot_general(
            jnp.concatenate([left[i] for i, _ in pairs], axis=0),
            jnp.concatenate([right[i] for _, i in pairs], axis=0),
            (((0,), (0,)), ((), ())),
            preferred_element_type=jnp.float32,
        )
        if more:
            now = []
            for i in range(per):
                fresh = []
                for w in range(wide):
                    spread = ahead_c[0][i] * row(done[0][w], 0)
                    for q in range(1, step):
                        spread = spread + ahead_c[q][i] * row(done[q // 8][w], q % 8)
                    base = ahead[i][w]
                    base = jnp.where(inside, 0.0, base) if w == w0 else base
                    fresh.append(base - spread)
                now.append(fresh)
        for g in range(size // 8):
            for w in range(wide):
                if g0 <= g < g0 + per:
                    value = done[g - g0][w]
                elif more and g0 + per <= g < g0 + 2 * per:
                    value = now[g - g0 - per][w]
                else:
                    value = tile(g, w)
                    value = jnp.where(inside, 0.0, value) if w == w0 else value
                    value = value - update[8 * g : 8 * g + 8, 128 * w : 128 * w + 128]
                a[8 * g : 8 * g + 8, 128 * w : 128 * w + 128] = value


def inverse_kernel(nj, nk, height_b, flipped, where, *refs):
    c_parts, refs = refs[:nk], refs[nk:]
    b_parts, refs = refs[:nk], refs[nk:]
    out, b_all = refs

    def gram(x, contracted):
        dims = (((contracted,), (contracted,)), ((), ()))
        return lax.dot_general(x, x, dims, preferred_element_type=jnp.float32)

    for t in range(nk):
        if flipped:
            at = pl.multiple_of(wrap(where[1] - t, nk) * height_b, height_b)
            b_all[:, pl.ds(at, height_b), :] = b_parts[t][...]
        else:
            at = pl.multiple_of(wrap(where[1] - t, nk) * 128, 128)
            b_all[:, :, pl.ds(at, 128)] = b_parts[t][...]
    if flipped:
        gram_b = sum(gram(b_all[s], 1) for s in range(nj))
    else:
        gram_b = gram(b_all[...].reshape(nj * height_b, out.shape[1]), 0)
    gram_c = sum(gram(part[...], 1) for part in c_parts)
    diagonal = lax.broadcasted_iota(jnp.int32, out.shape, 0) == lax.broadcasted_iota(
        jnp.int32, out.shape, 1
    )
    out[...] = gram_b * gram_c + jnp.where(diagonal, ridge_weight, 0.0)
    invert(out)


def solve_kernel(*refs):
    rows, (inverse, out) = refs[:-2], refs[-2:]
    mine = rows[0][...]
    for r in rows[1:]:
        mine = mine + r[...]
    out[...] = jnp.dot(mine, inverse[...], precision=exact, preferred_element_type=jnp.float32)


def body(tensor, factor_b, factor_c):
    nj, nk = lax.axis_size("ja"), lax.axis_size("ka")
    where = jnp.stack([lax.axis_index("ja"), lax.axis_index("ka")]).astype(jnp.int32)
    rank = factor_b.shape[1] * nk
    flipped = factor_b.shape[1] % 128 != 0
    part_b = factor_b.T if flipped else factor_b
    height_b = part_b.shape[0]
    mine = jnp.concatenate([part_b, factor_c.T], axis=0)
    line = [mine] + [lax.ppermute(mine, "ja", shift(nj, s)) for s in range(1, nj)]
    b_parts = [mine] + [lax.ppermute(mine, "ka", shift(nk, t)) for t in range(1, nk)]
    held = fetch(where, tensor, nj, nk)
    total, away, c_own, b_own = mttkrp(where, held, line, b_parts, height_b, flipped, rank)
    c_parts = [c_own] + [lax.ppermute(c_own, "ka", shift(nk, t)) for t in range(1, nk)]
    b_parts = [b_own] + [lax.ppermute(b_own, "ka", shift(nk, t)) for t in range(1, nk)]
    for t in range(1, nk):
        total = total + lax.ppermute(away[t - 1], "ka", shift(nk, t))
    rows = [total[0]] + [lax.ppermute(total[u], "ja", shift(nj, u)) for u in range(1, nj)]
    b_shape = (nj, rank, part_b.shape[1]) if flipped else (nj, height_b, rank)
    inverse = pl.pallas_call(
        functools.partial(inverse_kernel, nj, nk, height_b, flipped),
        out_shape=jax.ShapeDtypeStruct((rank, rank), jnp.float32),
        in_specs=[smem] + [vmem] * (2 * nk),
        out_specs=vmem,
        scratch_shapes=[pltpu.VMEM(b_shape, factor_b.dtype)],
        compiler_params=pltpu.CompilerParams(vmem_limit_bytes=20 * 2**20),
        cost_estimate=pl.CostEstimate(flops=10**10, bytes_accessed=2**20, transcendentals=0),
    )(where, *c_parts, *b_parts)
    return pl.pallas_call(
        solve_kernel,
        out_shape=jax.ShapeDtypeStruct((rows[0].shape[0], rank), jnp.float32),
        in_specs=[vmem] * (len(rows) + 1),
        out_specs=vmem,
        compiler_params=pltpu.CompilerParams(vmem_limit_bytes=20 * 2**20),
        cost_estimate=pl.CostEstimate(flops=10**8, bytes_accessed=2**19, transcendentals=0),
    )(*rows, inverse)


def solution(mesh):
    placed = (P("ia", "ja", "ka"), P("ja", "ka"), P("ka", "ja"))
    return jax.shard_map(
        body, mesh=mesh, in_specs=placed, out_specs=P(("ia", "ja", "ka"), None), check_vma=False
    )
```

```python
import functools

import jax
import jax.numpy as jnp
from jax import lax
from jax.experimental import pallas as pl
from jax.experimental.pallas import tpu as pltpu
from jax.sharding import PartitionSpec as P

ridge_weight = 0.1
exact = lax.Precision.HIGHEST
vmem = pl.BlockSpec(memory_space=pltpu.VMEM)
smem = pl.BlockSpec(memory_space=pltpu.SMEM)
hbm = pl.BlockSpec(memory_space=pltpu.HBM)


def shift(n, s):
    return [(i, (i + s) % n) for i in range(n)]


def wrap(x, n):
    return lax.rem(x + n, n)


def owner(nj, nk, where, t, u):
    return lax.bitwise_xor(where[0], u) * nk + wrap(where[1] + t, nk)


def halving_order(nj):
    order = [0]
    while len(order) < nj:
        order = [2 * u for u in order] + [2 * u + 1 for u in order]
    return order


def fetch_kernel(nj, nk, where, block, held, arrived):
    owned = held.shape[2]
    copies = []
    for t in range(nk):
        for slot, u in enumerate(halving_order(nj)):
            first = pl.multiple_of(owner(nj, nk, where, t, u) * owned, owned)
            copies.append(
                pltpu.make_async_copy(
                    block.at[pl.ds(first, owned)], held.at[t, slot], arrived.at[t * nj + slot]
                )
            )
    for copy in copies:
        copy.start()
    for copy in copies:
        copy.wait()


def fetch(where, tensor, nj, nk):
    rows, width_j, width_k = tensor.shape
    owned = rows // (nj * nk)
    return pl.pallas_call(
        functools.partial(fetch_kernel, nj, nk),
        out_shape=jax.ShapeDtypeStruct((nk, nj, owned, width_j, width_k), tensor.dtype),
        in_specs=[smem, hbm],
        out_specs=vmem,
        scratch_shapes=[pltpu.SemaphoreType.DMA((nj * nk,))],
        compiler_params=pltpu.CompilerParams(vmem_limit_bytes=42 * 2**20),
        cost_estimate=pl.CostEstimate(
            flops=4 * 10**9, bytes_accessed=2 * rows * width_j * width_k, transcendentals=0
        ),
    )(where, tensor)


def contract(held, t, out, c_wide, b_wide):
    nj, owned = held.shape[1], held.shape[2]

    for u in range(nj):
        sums = []
        for i in range(owned):
            inner = jnp.dot(held[t, u, i], c_wide, preferred_element_type=jnp.float32)
            sums.append(jnp.sum(inner * b_wide, axis=0, keepdims=True))
        out[u] = jnp.concatenate(sums, axis=0)


def away_kernel(nj, nk, height_b, flipped, where, held, *refs):
    line, refs = refs[:nj], refs[nj:]
    b_parts, refs = refs[:nk], refs[nk:]
    out, c_out, b_out, c_cols, b_cols, b_rows = refs
    width_c = line[0].shape[0] - height_b
    for s in range(nj):
        at = pl.multiple_of(wrap(where[0] - s, nj) * width_c, width_c)
        c_out[pl.ds(at, width_c), :] = line[s][height_b:, :]
        b_out[s] = line[s][:height_b, :]
    for t in range(nk):
        if flipped:
            at = pl.multiple_of(wrap(where[1] - t, nk) * height_b, height_b)
            b_rows[pl.ds(at, height_b), :] = b_parts[t][:height_b, :]
        else:
            at = pl.multiple_of(wrap(where[1] - t, nk) * 128, 128)
            b_rows[:, pl.ds(at, 128)] = b_parts[t][:height_b, :]
    c_cols[...] = c_out[...].T
    b_cols[...] = (b_rows[...].T if flipped else b_rows[...]).astype(jnp.float32)
    for t in range(1, nk):
        contract(held, t, out.at[t - 1], c_cols[...], b_cols[...])


def home_kernel(held, c_cols, b_cols, out):
    contract(held, 0, out, c_cols[...], b_cols[...])


def mttkrp(where, held, line, b_parts, height_b, flipped, rank):
    nk, nj, owned, width_j, width_k = held.shape
    flops = 2 * nj * owned * width_j * width_k * rank
    params = pltpu.CompilerParams(vmem_limit_bytes=20 * 2**20)

    def cost(count):
        return pl.CostEstimate(flops=count * flops, bytes_accessed=2**20, transcendentals=0)

    away, c_own, b_own, c_cols, b_cols = pl.pallas_call(
        functools.partial(away_kernel, nj, nk, height_b, flipped),
        out_shape=[
            jax.ShapeDtypeStruct((nk - 1, nj, owned, rank), jnp.float32),
            jax.ShapeDtypeStruct((rank, width_k), held.dtype),
            jax.ShapeDtypeStruct((nj, height_b, line[0].shape[1]), held.dtype),
            jax.ShapeDtypeStruct((width_k, rank), held.dtype),
            jax.ShapeDtypeStruct((width_j, rank), jnp.float32),
        ],
        in_specs=[smem] + [vmem] * (1 + nj + nk),
        out_specs=[vmem] * 5,
        scratch_shapes=[pltpu.VMEM((rank, width_j) if flipped else (width_j, rank), held.dtype)],
        compiler_params=params,
        cost_estimate=cost(nk - 1),
    )(where, held, *line, *b_parts)
    home = pl.pallas_call(
        home_kernel,
        out_shape=jax.ShapeDtypeStruct((nj, owned, rank), jnp.float32),
        in_specs=[vmem] * 3,
        out_specs=vmem,
        compiler_params=params,
        cost_estimate=cost(1),
    )(held, c_cols, b_cols)
    return home, away, c_own, b_own


def column(x, q):
    return jnp.broadcast_to(x[:, q : q + 1], x.shape)


def row(x, q):
    return jnp.broadcast_to(x[q : q + 1, :], x.shape)


def thirds(x):
    high = x.astype(jnp.bfloat16)
    x = x - high.astype(jnp.float32)
    middle = x.astype(jnp.bfloat16)
    return high, middle, (x - middle.astype(jnp.float32)).astype(jnp.bfloat16)


def stack(tiles):
    return jnp.concatenate([jnp.concatenate(r, axis=1) for r in tiles], axis=0)


def invert(a, begin, end, step=16):
    size = a.shape[0]
    wide, per = size // 128, step // 8
    lane = lax.broadcasted_iota(jnp.int32, (8, 128), 1)
    sub = lax.broadcasted_iota(jnp.int32, (8, 128), 0)

    def tile(g, w):
        return a[8 * g : 8 * g + 8, 128 * w : 128 * w + 128]

    def columns(rows, w, first):
        return [[column(r[w], first + q) for r in rows] for q in range(step)]

    now = [[tile(begin // 8 + g, w) for w in range(wide)] for g in range(per)]
    for first in range(begin, end, step):
        g0, w0, lane0 = first // 8, first // 128, first % 128
        inside = (lane >= lane0) & (lane < lane0 + step)
        more = first + step < size
        panel = [list(r) for r in now]
        c = columns(now, w0, lane0)
        if more:
            ahead = [[tile(g0 + per + i, w) for w in range(wide)] for i in range(per)]
            ahead_c = columns(ahead, w0, lane0)
        scale = [jnp.zeros((8, 128), jnp.float32)] * per
        pivot = row(c[0][0], 0)
        for q in range(step):
            gq, sq = q // 8, q % 8
            here = sub == sq
            inv = 1.0 / pivot
            scale[gq] = jnp.where(here, inv, scale[gq])
            if q + 1 < step:
                gn, sn = (q + 1) // 8, (q + 1) % 8
                product = row(c[q][gn], sn) * row(c[q + 1][gq], sq)
                pivot = row(c[q + 1][gn], sn) - product * inv
            factor = [jnp.where(here, 0.0, c[q][i]) if i == gq else c[q][i] for i in range(per)]
            for i in range(per):
                unit = jnp.where(here, 1.0, 0.0) if i == gq else 0.0
                panel[i][w0] = jnp.where(lane == lane0 + q, unit, panel[i][w0])
            for w in range(wide):
                scaled = row(panel[gq][w], sq) * inv
                for i in range(per):
                    panel[i][w] = panel[i][w] - factor[i] * scaled
            for p in range(q + 1, step):
                scaled = row(c[p][gq], sq) * inv
                for i in range(per):
                    c[p][i] = c[p][i] - factor[i] * scaled
        done = [[panel[i][w] * scale[i] for w in range(wide)] for i in range(per)]
        lanes = lax.broadcasted_iota(jnp.int32, (step, size), 1)
        left = stack(now)
        left = thirds(jnp.where(lanes < first, -left, left))
        right = thirds(stack(done))
        pairs = ((0, 0), (0, 1), (1, 0), (0, 2), (1, 1), (2, 0))
        update = lax.dot_general(
            jnp.concatenate([left[i] for i, _ in pairs], axis=0),
            jnp.concatenate([right[i] for _, i in pairs], axis=0),
            (((0,), (0,)), ((), ())),
            preferred_element_type=jnp.float32,
        )
        if more:
            now = []
            for i in range(per):
                fresh = []
                for w in range(wide):
                    spread = ahead_c[0][i] * row(done[0][w], 0)
                    for q in range(1, step):
                        spread = spread + ahead_c[q][i] * row(done[q // 8][w], q % 8)
                    base = ahead[i][w]
                    base = jnp.where(inside, 0.0, base) if w == w0 else base
                    fresh.append(base - spread)
                now.append(fresh)
        for g in range(size // 8):
            for w in range(wide):
                if g0 <= g < g0 + per:
                    value = done[g - g0][w]
                elif more and g0 + per <= g < g0 + 2 * per:
                    value = now[g - g0 - per][w]
                else:
                    value = tile(g, w)
                    value = jnp.where(inside, 0.0, value) if w == w0 else value
                    value = value - update[8 * g : 8 * g + 8, 128 * w : 128 * w + 128]
                a[8 * g : 8 * g + 8, 128 * w : 128 * w + 128] = value


def inverse_kernel(nj, nk, height_b, flipped, where, *refs):
    c_parts, refs = refs[:nk], refs[nk:]
    b_parts, refs = refs[:nk], refs[nk:]
    out, b_all = refs

    def gram(x, contracted):
        dims = (((contracted,), (contracted,)), ((), ()))
        return lax.dot_general(x, x, dims, preferred_element_type=jnp.float32)

    for t in range(nk):
        if flipped:
            at = pl.multiple_of(wrap(where[1] - t, nk) * height_b, height_b)
            b_all[:, pl.ds(at, height_b), :] = b_parts[t][...]
        else:
            at = pl.multiple_of(wrap(where[1] - t, nk) * 128, 128)
            b_all[:, :, pl.ds(at, 128)] = b_parts[t][...]
    if flipped:
        gram_b = sum(gram(b_all[s], 1) for s in range(nj))
    else:
        gram_b = gram(b_all[...].reshape(nj * height_b, out.shape[1]), 0)
    gram_c = sum(gram(part[...], 1) for part in c_parts)
    diagonal = lax.broadcasted_iota(jnp.int32, out.shape, 0) == lax.broadcasted_iota(
        jnp.int32, out.shape, 1
    )
    out[...] = gram_b * gram_c + jnp.where(diagonal, ridge_weight, 0.0)
    invert(out, 0, out.shape[0] // 2)


def rest_kernel(half_done, out):
    out[...] = half_done[...]
    invert(out, out.shape[0] // 2, out.shape[0])


def solve_kernel(kept, received, inverse, out):
    mine = kept[0] + received[0]
    out[...] = jnp.dot(mine, inverse[...], precision=exact, preferred_element_type=jnp.float32)


def body(tensor, factor_b, factor_c):
    nj, nk = lax.axis_size("ja"), lax.axis_size("ka")
    where = jnp.stack([lax.axis_index("ja"), lax.axis_index("ka")]).astype(jnp.int32)
    rank = factor_b.shape[1] * nk
    flipped = factor_b.shape[1] % 128 != 0
    part_b = factor_b.T if flipped else factor_b
    height_b = part_b.shape[0]
    mine = jnp.concatenate([part_b, factor_c.T], axis=0)
    line = [mine] + [lax.ppermute(mine, "ja", shift(nj, s)) for s in range(1, nj)]
    b_parts = [mine] + [lax.ppermute(mine, "ka", shift(nk, t)) for t in range(1, nk)]
    held = fetch(where, tensor, nj, nk)
    total, away, c_own, b_own = mttkrp(where, held, line, b_parts, height_b, flipped, rank)
    c_parts = [c_own] + [lax.ppermute(c_own, "ka", shift(nk, t)) for t in range(1, nk)]
    b_parts = [b_own] + [lax.ppermute(b_own, "ka", shift(nk, t)) for t in range(1, nk)]
    for t in range(1, nk):
        total = total + lax.ppermute(away[t - 1], "ka", shift(nk, t))
    b_shape = (nj, rank, part_b.shape[1]) if flipped else (nj, height_b, rank)
    params = pltpu.CompilerParams(vmem_limit_bytes=20 * 2**20)
    cost = pl.CostEstimate(flops=5 * 10**9, bytes_accessed=2**20, transcendentals=0)
    square = jax.ShapeDtypeStruct((rank, rank), jnp.float32)
    half_done = pl.pallas_call(
        functools.partial(inverse_kernel, nj, nk, height_b, flipped),
        out_shape=square,
        in_specs=[smem] + [vmem] * (2 * nk),
        out_specs=vmem,
        scratch_shapes=[pltpu.VMEM(b_shape, factor_b.dtype)],
        compiler_params=params,
        cost_estimate=cost,
    )(where, *c_parts, *b_parts)
    bit = 1
    while bit < nj:
        kept, sent = jnp.split(total, 2, axis=0)
        received = lax.ppermute(sent, "ja", [(i, i ^ bit) for i in range(nj)])
        total = kept if 2 * bit == nj else kept + received
        bit *= 2
    inverse = pl.pallas_call(
        rest_kernel,
        out_shape=square,
        in_specs=[vmem],
        out_specs=vmem,
        compiler_params=params,
        cost_estimate=cost,
    )(half_done)
    return pl.pallas_call(
        solve_kernel,
        out_shape=jax.ShapeDtypeStruct(kept.shape[1:], jnp.float32),
        in_specs=[vmem] * 3,
        out_specs=vmem,
        compiler_params=params,
        cost_estimate=pl.CostEstimate(flops=10**8, bytes_accessed=2**19, transcendentals=0),
    )(kept, received, inverse)


def solution(mesh):
    placed = (P("ia", "ja", "ka"), P("ja", "ka"), P("ka", "ja"))
    return jax.shard_map(
        body, mesh=mesh, in_specs=placed, out_specs=P(("ia", "ja", "ka"), None), check_vma=False
    )
```

```python
import functools

import jax
import jax.numpy as jnp
from jax import lax
from jax.experimental import pallas as pl
from jax.experimental.pallas import tpu as pltpu
from jax.sharding import PartitionSpec as P


ridge_weight = 0.1
exact = lax.Precision.HIGHEST
vmem = pl.BlockSpec(memory_space=pltpu.VMEM)
smem = pl.BlockSpec(memory_space=pltpu.SMEM)
hbm = pl.BlockSpec(memory_space=pltpu.HBM)


def shift(n, s):
    return [(i, (i + s) % n) for i in range(n)]


def wrap(x, n):
    return lax.rem(x + n, n)


def owner(nk, where, t, u):
    return lax.bitwise_xor(where[0], u) * nk + wrap(where[1] + t, nk)


def halving_order(nj):
    order = [0]
    while len(order) < nj:
        order = [2 * u for u in order] + [2 * u + 1 for u in order]
    return order


def copies(nj, nk, where, block, held, arrived, t):
    owned = held.shape[1]
    made = []
    for slot, u in enumerate(halving_order(nj)):
        first = pl.multiple_of(owner(nk, where, t, u) * owned, owned)
        rows = block.at[pl.ds(first, owned)]
        made.append(pltpu.make_async_copy(rows, held.at[slot], arrived.at[slot]))
    return made


def fetch_kernel(nj, nk, where, block, held, arrived):
    made = []
    for t in range(1, nk):
        made += copies(nj, nk, where, block, held.at[t - 1], arrived.at[t - 1], t)
    for copy in made:
        copy.start()
    for copy in made:
        copy.wait()


def fetch(where, tensor, nj, nk):
    rows, width_j, width_k = tensor.shape
    owned = rows // (nj * nk)
    return pl.pallas_call(
        functools.partial(fetch_kernel, nj, nk),
        out_shape=jax.ShapeDtypeStruct((nk - 1, nj, owned, width_j, width_k), tensor.dtype),
        in_specs=[smem, hbm],
        out_specs=vmem,
        scratch_shapes=[pltpu.SemaphoreType.DMA((nk - 1, nj))],
        compiler_params=pltpu.CompilerParams(vmem_limit_bytes=46 * 2**20),
        cost_estimate=pl.CostEstimate(
            flops=2 * 10**9, bytes_accessed=rows * width_j * width_k, transcendentals=0
        ),
    )(where, tensor)


def contract(held, out, c_wide, b_wide):
    count, owned = held.shape[0], held.shape[1]
    for u in range(count):
        sums = []
        for i in range(owned):
            inner = jnp.dot(held[u, i], c_wide, preferred_element_type=jnp.float32)
            sums.append(jnp.sum(inner * b_wide, axis=0, keepdims=True))
        out[u] = jnp.concatenate(sums, axis=0)


def away_kernel(nj, nk, height_b, flipped, where, block, held, *refs):
    line, refs = refs[:nj], refs[nj:]
    b_parts, refs = refs[:nk], refs[nk:]
    out, own, c_cols, b_cols, home_held, b_rows, arrived = refs
    rank = c_cols.shape[1]
    home = copies(nj, nk, where, block, home_held, arrived, 0)
    for copy in home:
        copy.start()
    width_c = line[0].shape[0] - height_b
    for s in range(nj):
        at = pl.multiple_of(wrap(where[0] - s, nj) * width_c, width_c)
        own[pl.ds(at, width_c), :] = line[s][height_b:, :]
        own[rank + s * height_b : rank + (s + 1) * height_b, :] = line[s][:height_b, :]
    for t in range(nk):
        if flipped:
            at = pl.multiple_of(wrap(where[1] - t, nk) * height_b, height_b)
            b_rows[pl.ds(at, height_b), :] = b_parts[t][:height_b, :]
        else:
            at = pl.multiple_of(wrap(where[1] - t, nk) * 128, 128)
            b_rows[:, pl.ds(at, 128)] = b_parts[t][:height_b, :]
    c_cols[...] = own[:rank, :].T
    b_cols[...] = (b_rows[...].T if flipped else b_rows[...]).astype(jnp.float32)
    for t in range(1, nk):
        contract(held.at[t - 1], out.at[t - 1], c_cols[...], b_cols[...])
    for copy in home:
        copy.wait()


def home_kernel(begin, count, held, c_cols, b_cols, out):
    contract(held.at[begin : begin + count], out, c_cols[...], b_cols[...])


def flops_of(rows, held, rank):
    return pl.CostEstimate(
        flops=2 * rows * held.shape[-2] * held.shape[-1] * rank,
        bytes_accessed=2**20,
        transcendentals=0,
    )


def contract_away(where, tensor, held, line, b_parts, height_b, flipped, rank):
    _, nj, owned, width_j, width_k = held.shape
    nk = len(b_parts)
    width = line[0].shape[1]
    return pl.pallas_call(
        functools.partial(away_kernel, nj, nk, height_b, flipped),
        out_shape=[
            jax.ShapeDtypeStruct((nk - 1, nj, owned, rank), jnp.float32),
            jax.ShapeDtypeStruct((rank + nj * height_b, width), held.dtype),
            jax.ShapeDtypeStruct((width_k, rank), held.dtype),
            jax.ShapeDtypeStruct((width_j, rank), jnp.float32),
            jax.ShapeDtypeStruct(held.shape[1:], held.dtype),
        ],
        in_specs=[smem, hbm] + [vmem] * (1 + nj + nk),
        out_specs=[vmem] * 5,
        scratch_shapes=[
            pltpu.VMEM((rank, width_j) if flipped else (width_j, rank), held.dtype),
            pltpu.SemaphoreType.DMA((nj,)),
        ],
        compiler_params=pltpu.CompilerParams(vmem_limit_bytes=44 * 2**20),
        cost_estimate=flops_of((nk - 1) * nj * owned, held, rank),
    )(where, tensor, held, *line, *b_parts)


def contract_home(begin, count, held, c_cols, b_cols):
    _, owned, _, _ = held.shape
    rank = c_cols.shape[1]
    return pl.pallas_call(
        functools.partial(home_kernel, begin, count),
        out_shape=jax.ShapeDtypeStruct((count, owned, rank), jnp.float32),
        in_specs=[vmem] * 3,
        out_specs=vmem,
        compiler_params=pltpu.CompilerParams(vmem_limit_bytes=20 * 2**20),
        cost_estimate=flops_of(count * owned, held, rank),
    )(held, c_cols, b_cols)


def column(x, q):
    return jnp.take_along_axis(x, jnp.full(x.shape, q, jnp.int32), axis=1)


def row(x, q):
    return jnp.broadcast_to(x[q : q + 1, :], x.shape)


def thirds(x):
    high = x.astype(jnp.bfloat16)
    x = x - high.astype(jnp.float32)
    middle = x.astype(jnp.bfloat16)
    return high, middle, (x - middle.astype(jnp.float32)).astype(jnp.bfloat16)


def stack(tiles):
    return jnp.concatenate([jnp.concatenate(r, axis=1) for r in tiles], axis=0)


def invert(a, begin, end, step=16):
    size = a.shape[0]
    wide, per = size // 128, step // 8
    lane = lax.broadcasted_iota(jnp.int32, (8, 128), 1)
    sub = lax.broadcasted_iota(jnp.int32, (8, 128), 0)

    def tile(g, w):
        return a[8 * g : 8 * g + 8, 128 * w : 128 * w + 128]

    def columns(rows, w, first):
        return [[column(r[w], first + q) for r in rows] for q in range(step)]

    now = [[tile(begin // 8 + g, w) for w in range(wide)] for g in range(per)]
    for first in range(begin, end, step):
        g0, w0, lane0 = first // 8, first // 128, first % 128
        inside = (lane >= lane0) & (lane < lane0 + step)
        more = first + step < size
        panel = [list(r) for r in now]
        c = columns(now, w0, lane0)
        if more:
            ahead = [[tile(g0 + per + i, w) for w in range(wide)] for i in range(per)]
            ahead_c = columns(ahead, w0, lane0)
        scale = [jnp.zeros((8, 128), jnp.float32)] * per
        pivot = row(c[0][0], 0)
        for i in range(per):
            unit = jnp.where(lane == sub + (lane0 + 8 * i), 1.0, 0.0)
            panel[i][w0] = jnp.where(inside, unit, panel[i][w0])
        for q in range(step):
            gq, sq = q // 8, q % 8
            here = sub == sq
            inv = 1.0 / pivot
            scale[gq] = jnp.where(here, inv, scale[gq])
            if q + 1 < step:
                gn, sn = (q + 1) // 8, (q + 1) % 8
                product = row(c[q][gn], sn) * row(c[q + 1][gq], sq)
                pivot = row(c[q + 1][gn], sn) - product * inv
            factor = [jnp.where(here, 0.0, c[q][i]) if i == gq else c[q][i] for i in range(per)]
            factor = [f * inv for f in factor]
            for p in range(q + 1, step):
                pivot_row = row(c[p][gq], sq)
                for i in range(per):
                    c[p][i] = c[p][i] - factor[i] * pivot_row
            for w in range(wide):
                pivot_row = row(panel[gq][w], sq)
                for i in range(per):
                    panel[i][w] = panel[i][w] - factor[i] * pivot_row
        done = [[panel[i][w] * scale[i] for w in range(wide)] for i in range(per)]
        lanes = lax.broadcasted_iota(jnp.int32, (step, size), 1)
        left = stack(now)
        left = thirds(jnp.where(lanes < first, -left, left))
        right = thirds(stack(done))
        pairs = ((0, 0), (0, 1), (1, 0), (0, 2), (1, 1), (2, 0))
        update = lax.dot_general(
            jnp.concatenate([left[i] for i, _ in pairs], axis=0),
            jnp.concatenate([right[i] for _, i in pairs], axis=0),
            (((0,), (0,)), ((), ())),
            preferred_element_type=jnp.float32,
        )
        if more:
            now = []
            for i in range(per):
                fresh = []
                for w in range(wide):
                    terms = [ahead_c[q][i] * row(done[q // 8][w], q % 8) for q in range(step)]
                    while len(terms) > 1:
                        terms = [x + y for x, y in zip(terms[::2], terms[1::2])]
                    spread = terms[0]
                    base = ahead[i][w]
                    base = jnp.where(inside, 0.0, base) if w == w0 else base
                    fresh.append(base - spread)
                now.append(fresh)
        for g in range(size // 8):
            for w in range(wide):
                if g0 <= g < g0 + per:
                    value = done[g - g0][w]
                elif more and g0 + per <= g < g0 + 2 * per:
                    value = now[g - g0 - per][w]
                else:
                    value = tile(g, w)
                    value = jnp.where(inside, 0.0, value) if w == w0 else value
                    value = value - update[8 * g : 8 * g + 8, 128 * w : 128 * w + 128]
                a[8 * g : 8 * g + 8, 128 * w : 128 * w + 128] = value


def inverse_kernel(nj, nk, height_b, flipped, blocks, where, *refs):
    owns, (out, b_all) = refs[:nk], refs[nk:]
    rank = out.shape[1]

    def gram(x, contracted):
        dims = (((contracted,), (contracted,)), ((), ()))
        return lax.dot_general(x, x, dims, preferred_element_type=jnp.float32)

    for t in range(nk):
        part = owns[t][rank:, :].reshape(nj, height_b, owns[t].shape[1])
        if flipped:
            at = pl.multiple_of(wrap(where[1] - t, nk) * height_b, height_b)
            b_all[:, pl.ds(at, height_b), :] = part
        else:
            at = pl.multiple_of(wrap(where[1] - t, nk) * 128, 128)
            b_all[:, :, pl.ds(at, 128)] = part
    if flipped:
        gram_b = sum(gram(b_all[s], 1) for s in range(nj))
    else:
        gram_b = gram(b_all[...].reshape(nj * height_b, rank), 0)
    gram_c = sum(gram(own[:rank, :], 1) for own in owns)
    diagonal = lax.broadcasted_iota(jnp.int32, out.shape, 0) == lax.broadcasted_iota(
        jnp.int32, out.shape, 1
    )
    out[...] = gram_b * gram_c + jnp.where(diagonal, ridge_weight, 0.0)
    invert(out, 0, blocks)


def rest_kernel(blocks, half_done, out):
    out[...] = half_done[...]
    invert(out, blocks, out.shape[0])


def solve_kernel(kept, received, inverse, out):
    mine = kept[0] + received[0]
    out[...] = jnp.dot(mine, inverse[...], precision=exact, preferred_element_type=jnp.float32)


def send(x, axis, n, s):
    return lax.ppermute(x, axis, shift(n, s))


def update(tensor, factor_b, factor_c):
    nj, nk = lax.axis_size("ja"), lax.axis_size("ka")
    where = jnp.stack([lax.axis_index("ja"), lax.axis_index("ka")]).astype(jnp.int32)
    rank = factor_b.shape[1] * nk
    flipped = factor_b.shape[1] % 128 != 0
    part_b = factor_b.T if flipped else factor_b
    height_b = part_b.shape[0]
    mine = jnp.concatenate([part_b, factor_c.T], axis=0)
    line = [mine] + [send(mine, "ja", nj, s) for s in range(1, nj)]
    b_parts = [mine] + [send(mine, "ka", nk, t) for t in range(1, nk)]
    held = fetch(where, tensor, nj, nk)
    away, own, c_cols, b_cols, held = contract_away(
        where, tensor, held, line, b_parts, height_b, flipped, rank
    )
    half = nj // 2
    sent = contract_home(half, half, held, c_cols, b_cols)
    for t in range(1, nk):
        received = send(away[t - 1], "ka", nk, t)
        sent = sent + received[half:]
        away_kept = received[:half] if t == 1 else away_kept + received[:half]
    owns = [own] + [send(own, "ka", nk, t) for t in range(1, nk)]
    kept = contract_home(0, half, held, c_cols, b_cols)
    kept = kept + away_kept
    params = pltpu.CompilerParams(vmem_limit_bytes=20 * 2**20)
    cost = pl.CostEstimate(flops=5 * 10**9, bytes_accessed=2**20, transcendentals=0)
    square = jax.ShapeDtypeStruct((rank, rank), jnp.float32)
    blocks = rank // 64 * 16
    b_shape = (nj, rank, mine.shape[1]) if flipped else (nj, height_b, rank)
    half_done = pl.pallas_call(
        functools.partial(inverse_kernel, nj, nk, height_b, flipped, blocks),
        out_shape=square,
        in_specs=[smem] + [vmem] * nk,
        out_specs=vmem,
        scratch_shapes=[pltpu.VMEM(b_shape, mine.dtype)],
        compiler_params=params,
        cost_estimate=cost,
    )(where, *owns)
    bit = 1
    while True:
        received = lax.ppermute(sent, "ja", [(i, i ^ bit) for i in range(nj)])
        bit *= 2
        if bit == nj:
            break
        kept, sent = jnp.split(kept + received, 2, axis=0)
    inverse = pl.pallas_call(
        functools.partial(rest_kernel, blocks),
        out_shape=square,
        in_specs=[vmem],
        out_specs=vmem,
        compiler_params=params,
        cost_estimate=cost,
    )(half_done)
    return pl.pallas_call(
        solve_kernel,
        out_shape=jax.ShapeDtypeStruct(kept.shape[1:], jnp.float32),
        in_specs=[vmem] * 3,
        out_specs=vmem,
        compiler_params=params,
        cost_estimate=pl.CostEstimate(flops=10**8, bytes_accessed=2**19, transcendentals=0),
    )(kept, received, inverse)


def solution(mesh):
    placed = (P("ia", "ja", "ka"), P("ja", "ka"), P("ka", "ja"))
    return jax.shard_map(
        update, mesh=mesh, in_specs=placed, out_specs=P(("ia", "ja", "ka"), None), check_vma=False
    )
```

```python
import functools

import jax
import jax.numpy as jnp
from jax import lax
from jax.experimental import pallas as pl
from jax.experimental.pallas import tpu as pltpu
from jax.sharding import PartitionSpec as P


ridge_weight = 0.1
exact = lax.Precision.HIGHEST
vmem = pl.BlockSpec(memory_space=pltpu.VMEM)
smem = pl.BlockSpec(memory_space=pltpu.SMEM)
hbm = pl.BlockSpec(memory_space=pltpu.HBM)


def shift(n, s):
    return [(i, (i + s) % n) for i in range(n)]


def wrap(x, n):
    return lax.rem(x + n, n)


def owner(nk, where, t, u):
    return lax.bitwise_xor(where[0], u) * nk + wrap(where[1] + t, nk)


def halving_order(nj):
    order = [0]
    while len(order) < nj:
        order = [2 * u for u in order] + [2 * u + 1 for u in order]
    return order


def fetch_kernel(nj, nk, where, block, held, arrived):
    owned = held.shape[2]
    copies = []
    for t in range(nk):
        for slot, u in enumerate(halving_order(nj)):
            first = pl.multiple_of(owner(nk, where, t, u) * owned, owned)
            rows = block.at[pl.ds(first, owned)]
            copies.append(pltpu.make_async_copy(rows, held.at[t, slot], arrived.at[t, slot]))
    for copy in copies:
        copy.start()
    for copy in copies:
        copy.wait()


def fetch(where, tensor, nj, nk):
    rows, width_j, width_k = tensor.shape
    owned = rows // (nj * nk)
    return pl.pallas_call(
        functools.partial(fetch_kernel, nj, nk),
        out_shape=jax.ShapeDtypeStruct((nk, nj, owned, width_j, width_k), tensor.dtype),
        in_specs=[smem, hbm],
        out_specs=vmem,
        scratch_shapes=[pltpu.SemaphoreType.DMA((nk, nj))],
        compiler_params=pltpu.CompilerParams(vmem_limit_bytes=42 * 2**20),
        cost_estimate=pl.CostEstimate(
            flops=4 * 10**9, bytes_accessed=2 * rows * width_j * width_k, transcendentals=0
        ),
    )(where, tensor)


def contract(held, out, c_wide, b_wide):
    count, owned = held.shape[0], held.shape[1]
    for u in range(count):
        sums = []
        for i in range(owned):
            inner = jnp.dot(held[u, i], c_wide, preferred_element_type=jnp.float32)
            sums.append(jnp.sum(inner * b_wide, axis=0, keepdims=True))
        out[u] = jnp.concatenate(sums, axis=0)


def away_kernel(nj, nk, height_b, flipped, where, held, *refs):
    line, refs = refs[:nj], refs[nj:]
    b_parts, refs = refs[:nk], refs[nk:]
    out, own, c_cols, b_cols, b_rows = refs
    rank = c_cols.shape[1]
    width_c = line[0].shape[0] - height_b
    for s in range(nj):
        at = pl.multiple_of(wrap(where[0] - s, nj) * width_c, width_c)
        own[pl.ds(at, width_c), :] = line[s][height_b:, :]
        own[rank + s * height_b : rank + (s + 1) * height_b, :] = line[s][:height_b, :]
    for t in range(nk):
        if flipped:
            at = pl.multiple_of(wrap(where[1] - t, nk) * height_b, height_b)
            b_rows[pl.ds(at, height_b), :] = b_parts[t][:height_b, :]
        else:
            at = pl.multiple_of(wrap(where[1] - t, nk) * 128, 128)
            b_rows[:, pl.ds(at, 128)] = b_parts[t][:height_b, :]
    c_cols[...] = own[:rank, :].T
    b_cols[...] = (b_rows[...].T if flipped else b_rows[...]).astype(jnp.float32)
    for t in range(1, nk):
        contract(held.at[t], out.at[t - 1], c_cols[...], b_cols[...])


def home_kernel(begin, count, held, c_cols, b_cols, out):
    contract(held.at[0, begin : begin + count], out, c_cols[...], b_cols[...])


def flops_of(rows, held, rank):
    return pl.CostEstimate(
        flops=2 * rows * held.shape[-2] * held.shape[-1] * rank,
        bytes_accessed=2**20,
        transcendentals=0,
    )


def contract_away(where, held, line, b_parts, height_b, flipped, rank):
    nk, nj, owned, width_j, width_k = held.shape
    width = line[0].shape[1]
    return pl.pallas_call(
        functools.partial(away_kernel, nj, nk, height_b, flipped),
        out_shape=[
            jax.ShapeDtypeStruct((nk - 1, nj, owned, rank), jnp.float32),
            jax.ShapeDtypeStruct((rank + nj * height_b, width), held.dtype),
            jax.ShapeDtypeStruct((width_k, rank), held.dtype),
            jax.ShapeDtypeStruct((width_j, rank), jnp.float32),
        ],
        in_specs=[smem] + [vmem] * (1 + nj + nk),
        out_specs=[vmem] * 4,
        scratch_shapes=[pltpu.VMEM((rank, width_j) if flipped else (width_j, rank), held.dtype)],
        compiler_params=pltpu.CompilerParams(vmem_limit_bytes=20 * 2**20),
        cost_estimate=flops_of((nk - 1) * nj * owned, held, rank),
    )(where, held, *line, *b_parts)


def contract_home(begin, count, held, c_cols, b_cols):
    _, _, owned, _, _ = held.shape
    rank = c_cols.shape[1]
    return pl.pallas_call(
        functools.partial(home_kernel, begin, count),
        out_shape=jax.ShapeDtypeStruct((count, owned, rank), jnp.float32),
        in_specs=[vmem] * 3,
        out_specs=vmem,
        compiler_params=pltpu.CompilerParams(vmem_limit_bytes=20 * 2**20),
        cost_estimate=flops_of(count * owned, held, rank),
    )(held, c_cols, b_cols)


def column(x, q):
    return jnp.take_along_axis(x, jnp.full(x.shape, q, jnp.int32), axis=1)


def row(x, q):
    return jnp.broadcast_to(x[q : q + 1, :], x.shape)


def thirds(x):
    high = x.astype(jnp.bfloat16)
    x = x - high.astype(jnp.float32)
    middle = x.astype(jnp.bfloat16)
    return high, middle, (x - middle.astype(jnp.float32)).astype(jnp.bfloat16)


def stack(tiles):
    return jnp.concatenate([jnp.concatenate(r, axis=1) for r in tiles], axis=0)


def invert(a, begin, end, step=16):
    size = a.shape[0]
    wide, per = size // 128, step // 8
    lane = lax.broadcasted_iota(jnp.int32, (8, 128), 1)
    sub = lax.broadcasted_iota(jnp.int32, (8, 128), 0)

    def tile(g, w):
        return a[8 * g : 8 * g + 8, 128 * w : 128 * w + 128]

    def columns(rows, w, first):
        return [[column(r[w], first + q) for r in rows] for q in range(step)]

    now = [[tile(begin // 8 + g, w) for w in range(wide)] for g in range(per)]
    for first in range(begin, end, step):
        g0, w0, lane0 = first // 8, first // 128, first % 128
        inside = (lane >= lane0) & (lane < lane0 + step)
        more = first + step < size
        panel = [list(r) for r in now]
        c = columns(now, w0, lane0)
        if more:
            ahead = [[tile(g0 + per + i, w) for w in range(wide)] for i in range(per)]
            ahead_c = columns(ahead, w0, lane0)
        scale = [jnp.zeros((8, 128), jnp.float32)] * per
        pivot = row(c[0][0], 0)
        for i in range(per):
            unit = jnp.where(lane == sub + (lane0 + 8 * i), 1.0, 0.0)
            panel[i][w0] = jnp.where(inside, unit, panel[i][w0])
        for q in range(step):
            gq, sq = q // 8, q % 8
            here = sub == sq
            inv = 1.0 / pivot
            scale[gq] = jnp.where(here, inv, scale[gq])
            if q + 1 < step:
                gn, sn = (q + 1) // 8, (q + 1) % 8
                product = row(c[q][gn], sn) * row(c[q + 1][gq], sq)
                pivot = row(c[q + 1][gn], sn) - product * inv
            factor = [jnp.where(here, 0.0, c[q][i]) if i == gq else c[q][i] for i in range(per)]
            factor = [f * inv for f in factor]
            for p in range(q + 1, step):
                pivot_row = row(c[p][gq], sq)
                for i in range(per):
                    c[p][i] = c[p][i] - factor[i] * pivot_row
            for w in range(wide):
                pivot_row = row(panel[gq][w], sq)
                for i in range(per):
                    panel[i][w] = panel[i][w] - factor[i] * pivot_row
        done = [[panel[i][w] * scale[i] for w in range(wide)] for i in range(per)]
        lanes = lax.broadcasted_iota(jnp.int32, (step, size), 1)
        left = stack(now)
        left = thirds(jnp.where(lanes < first, -left, left))
        right = thirds(stack(done))
        pairs = ((0, 0), (0, 1), (1, 0), (0, 2), (1, 1), (2, 0))
        update = lax.dot_general(
            jnp.concatenate([left[i] for i, _ in pairs], axis=0),
            jnp.concatenate([right[i] for _, i in pairs], axis=0),
            (((0,), (0,)), ((), ())),
            preferred_element_type=jnp.float32,
        )
        if more:
            now = []
            for i in range(per):
                fresh = []
                for w in range(wide):
                    terms = [ahead_c[q][i] * row(done[q // 8][w], q % 8) for q in range(step)]
                    while len(terms) > 1:
                        terms = [x + y for x, y in zip(terms[::2], terms[1::2])]
                    spread = terms[0]
                    base = ahead[i][w]
                    base = jnp.where(inside, 0.0, base) if w == w0 else base
                    fresh.append(base - spread)
                now.append(fresh)
        for g in range(size // 8):
            for w in range(wide):
                if g0 <= g < g0 + per:
                    value = done[g - g0][w]
                elif more and g0 + per <= g < g0 + 2 * per:
                    value = now[g - g0 - per][w]
                else:
                    value = tile(g, w)
                    value = jnp.where(inside, 0.0, value) if w == w0 else value
                    value = value - update[8 * g : 8 * g + 8, 128 * w : 128 * w + 128]
                a[8 * g : 8 * g + 8, 128 * w : 128 * w + 128] = value


def inverse_kernel(nj, nk, height_b, flipped, blocks, where, *refs):
    owns, (out, b_all) = refs[:nk], refs[nk:]
    rank = out.shape[1]

    def gram(x, contracted):
        dims = (((contracted,), (contracted,)), ((), ()))
        return lax.dot_general(x, x, dims, preferred_element_type=jnp.float32)

    for t in range(nk):
        part = owns[t][rank:, :].reshape(nj, height_b, owns[t].shape[1])
        if flipped:
            at = pl.multiple_of(wrap(where[1] - t, nk) * height_b, height_b)
            b_all[:, pl.ds(at, height_b), :] = part
        else:
            at = pl.multiple_of(wrap(where[1] - t, nk) * 128, 128)
            b_all[:, :, pl.ds(at, 128)] = part
    if flipped:
        gram_b = sum(gram(b_all[s], 1) for s in range(nj))
    else:
        gram_b = gram(b_all[...].reshape(nj * height_b, rank), 0)
    gram_c = sum(gram(own[:rank, :], 1) for own in owns)
    diagonal = lax.broadcasted_iota(jnp.int32, out.shape, 0) == lax.broadcasted_iota(
        jnp.int32, out.shape, 1
    )
    out[...] = gram_b * gram_c + jnp.where(diagonal, ridge_weight, 0.0)
    invert(out, 0, blocks)


def rest_kernel(blocks, half_done, out):
    out[...] = half_done[...]
    invert(out, blocks, out.shape[0])


def solve_kernel(kept, received, inverse, out):
    mine = kept[0] + received[0]
    out[...] = jnp.dot(mine, inverse[...], precision=exact, preferred_element_type=jnp.float32)


def send(x, axis, n, s):
    return lax.ppermute(x, axis, shift(n, s))


def update(tensor, factor_b, factor_c):
    nj, nk = lax.axis_size("ja"), lax.axis_size("ka")
    where = jnp.stack([lax.axis_index("ja"), lax.axis_index("ka")]).astype(jnp.int32)
    rank = factor_b.shape[1] * nk
    flipped = factor_b.shape[1] % 128 != 0
    part_b = factor_b.T if flipped else factor_b
    height_b = part_b.shape[0]
    mine = jnp.concatenate([part_b, factor_c.T], axis=0)
    line = [mine] + [send(mine, "ja", nj, s) for s in range(1, nj)]
    b_parts = [mine] + [send(mine, "ka", nk, t) for t in range(1, nk)]
    held = fetch(where, tensor, nj, nk)
    away, own, c_cols, b_cols = contract_away(
        where, held, line, b_parts, height_b, flipped, rank
    )
    half = nj // 2
    sent = contract_home(half, half, held, c_cols, b_cols)
    for t in range(1, nk):
        received = send(away[t - 1], "ka", nk, t)
        sent = sent + received[half:]
        away_kept = received[:half] if t == 1 else away_kept + received[:half]
    owns = [own] + [send(own, "ka", nk, t) for t in range(1, nk)]
    kept = contract_home(0, half, held, c_cols, b_cols)
    kept = kept + away_kept
    params = pltpu.CompilerParams(vmem_limit_bytes=20 * 2**20)
    cost = pl.CostEstimate(flops=5 * 10**9, bytes_accessed=2**20, transcendentals=0)
    square = jax.ShapeDtypeStruct((rank, rank), jnp.float32)
    blocks = rank // 64 * 16
    b_shape = (nj, rank, mine.shape[1]) if flipped else (nj, height_b, rank)
    half_done = pl.pallas_call(
        functools.partial(inverse_kernel, nj, nk, height_b, flipped, blocks),
        out_shape=square,
        in_specs=[smem] + [vmem] * nk,
        out_specs=vmem,
        scratch_shapes=[pltpu.VMEM(b_shape, mine.dtype)],
        compiler_params=params,
        cost_estimate=cost,
    )(where, *owns)
    bit = 1
    while True:
        received = lax.ppermute(sent, "ja", [(i, i ^ bit) for i in range(nj)])
        bit *= 2
        if bit == nj:
            break
        kept, sent = jnp.split(kept + received, 2, axis=0)
    inverse = pl.pallas_call(
        functools.partial(rest_kernel, blocks),
        out_shape=square,
        in_specs=[vmem],
        out_specs=vmem,
        compiler_params=params,
        cost_estimate=cost,
    )(half_done)
    return pl.pallas_call(
        solve_kernel,
        out_shape=jax.ShapeDtypeStruct(kept.shape[1:], jnp.float32),
        in_specs=[vmem] * 3,
        out_specs=vmem,
        compiler_params=params,
        cost_estimate=pl.CostEstimate(flops=10**8, bytes_accessed=2**19, transcendentals=0),
    )(kept, received, inverse)


def solution(mesh):
    placed = (P("ia", "ja", "ka"), P("ja", "ka"), P("ka", "ja"))
    return jax.shard_map(
        update, mesh=mesh, in_specs=placed, out_specs=P(("ia", "ja", "ka"), None), check_vma=False
    )
```

```python
import functools

import jax
import jax.numpy as jnp
from jax import lax
from jax.experimental import pallas as pl
from jax.experimental.pallas import tpu as pltpu
from jax.sharding import PartitionSpec as P


ridge_weight = 0.1
exact = lax.Precision.HIGHEST
vmem = pl.BlockSpec(memory_space=pltpu.VMEM)
smem = pl.BlockSpec(memory_space=pltpu.SMEM)
hbm = pl.BlockSpec(memory_space=pltpu.HBM)


def shift(n, s):
    return [(i, (i + s) % n) for i in range(n)]


def wrap(x, n):
    return lax.rem(x + n, n)


def owner(nk, where, t, u):
    return lax.bitwise_xor(where[0], u) * nk + wrap(where[1] + t, nk)


def halving_order(nj):
    order = [0]
    while len(order) < nj:
        order = [2 * u for u in order] + [2 * u + 1 for u in order]
    return order


def fetch_kernel(nj, nk, where, block, held, arrived):
    owned = held.shape[2]
    copies = []
    for t in range(nk):
        for slot, u in enumerate(halving_order(nj)):
            first = pl.multiple_of(owner(nk, where, t, u) * owned, owned)
            rows = block.at[pl.ds(first, owned)]
            copies.append(pltpu.make_async_copy(rows, held.at[t, slot], arrived.at[t, slot]))
    for copy in copies:
        copy.start()
    for copy in copies:
        copy.wait()


def fetch(where, tensor, nj, nk):
    rows, width_j, width_k = tensor.shape
    owned = rows // (nj * nk)
    return pl.pallas_call(
        functools.partial(fetch_kernel, nj, nk),
        out_shape=jax.ShapeDtypeStruct((nk, nj, owned, width_j, width_k), tensor.dtype),
        in_specs=[smem, hbm],
        out_specs=vmem,
        scratch_shapes=[pltpu.SemaphoreType.DMA((nk, nj))],
        compiler_params=pltpu.CompilerParams(vmem_limit_bytes=42 * 2**20),
        cost_estimate=pl.CostEstimate(
            flops=4 * 10**9, bytes_accessed=2 * rows * width_j * width_k, transcendentals=0
        ),
    )(where, tensor)


def contract(held, out, c_wide, b_wide):
    count, owned = held.shape[0], held.shape[1]
    for u in range(count):
        sums = []
        for i in range(owned):
            inner = jnp.dot(held[u, i], c_wide, preferred_element_type=jnp.float32)
            sums.append(jnp.sum(inner * b_wide, axis=0, keepdims=True))
        out[u] = jnp.concatenate(sums, axis=0)


def away_kernel(nj, nk, height_b, flipped, where, held, *refs):
    line, refs = refs[:nj], refs[nj:]
    b_parts, refs = refs[:nk], refs[nk:]
    out, own, c_cols, b_cols, b_rows = refs
    rank = c_cols.shape[1]
    width_c = line[0].shape[0] - height_b
    for s in range(nj):
        at = pl.multiple_of(wrap(where[0] - s, nj) * width_c, width_c)
        own[pl.ds(at, width_c), :] = line[s][height_b:, :]
        own[rank + s * height_b : rank + (s + 1) * height_b, :] = line[s][:height_b, :]
    for t in range(nk):
        if flipped:
            at = pl.multiple_of(wrap(where[1] - t, nk) * height_b, height_b)
            b_rows[pl.ds(at, height_b), :] = b_parts[t][:height_b, :]
        else:
            at = pl.multiple_of(wrap(where[1] - t, nk) * 128, 128)
            b_rows[:, pl.ds(at, 128)] = b_parts[t][:height_b, :]
    c_cols[...] = own[:rank, :].T
    b_cols[...] = (b_rows[...].T if flipped else b_rows[...]).astype(jnp.float32)
    for t in range(1, nk):
        contract(held.at[t, nj // 2 :], out.at[t - 1], c_cols[...], b_cols[...])


def rows_kernel(turns, begin, count, held, c_cols, b_cols, out):
    for slot, t in enumerate(turns):
        contract(held.at[t, begin : begin + count], out.at[slot], c_cols[...], b_cols[...])


def flops_of(rows, held, rank):
    return pl.CostEstimate(
        flops=2 * rows * held.shape[-2] * held.shape[-1] * rank,
        bytes_accessed=2**20,
        transcendentals=0,
    )


def contract_away(where, held, line, b_parts, height_b, flipped, rank):
    nk, nj, owned, width_j, width_k = held.shape
    width = line[0].shape[1]
    return pl.pallas_call(
        functools.partial(away_kernel, nj, nk, height_b, flipped),
        out_shape=[
            jax.ShapeDtypeStruct((nk - 1, nj // 2, owned, rank), jnp.float32),
            jax.ShapeDtypeStruct((rank + nj * height_b, width), held.dtype),
            jax.ShapeDtypeStruct((width_k, rank), held.dtype),
            jax.ShapeDtypeStruct((width_j, rank), jnp.float32),
        ],
        in_specs=[smem] + [vmem] * (1 + nj + nk),
        out_specs=[vmem] * 4,
        scratch_shapes=[pltpu.VMEM((rank, width_j) if flipped else (width_j, rank), held.dtype)],
        compiler_params=pltpu.CompilerParams(vmem_limit_bytes=20 * 2**20),
        cost_estimate=flops_of((nk - 1) * nj * owned // 2, held, rank),
    )(where, held, *line, *b_parts)


def contract_rows(turns, begin, count, held, c_cols, b_cols):
    owned, rank = held.shape[2], c_cols.shape[1]
    return pl.pallas_call(
        functools.partial(rows_kernel, turns, begin, count),
        out_shape=jax.ShapeDtypeStruct((len(turns), count, owned, rank), jnp.float32),
        in_specs=[vmem] * 3,
        out_specs=vmem,
        compiler_params=pltpu.CompilerParams(vmem_limit_bytes=20 * 2**20),
        cost_estimate=flops_of(len(turns) * count * owned, held, rank),
    )(held, c_cols, b_cols)


def column(x, q):
    return jnp.take_along_axis(x, jnp.full(x.shape, q, jnp.int32), axis=1)


def row(x, q):
    return jnp.broadcast_to(x[q : q + 1, :], x.shape)


def thirds(x):
    high = x.astype(jnp.bfloat16)
    x = x - high.astype(jnp.float32)
    middle = x.astype(jnp.bfloat16)
    return high, middle, (x - middle.astype(jnp.float32)).astype(jnp.bfloat16)


def stack(tiles):
    return jnp.concatenate([jnp.concatenate(r, axis=1) for r in tiles], axis=0)


def invert(a, begin, end, step=16):
    size = a.shape[0]
    wide, per = size // 128, step // 8
    lane = lax.broadcasted_iota(jnp.int32, (8, 128), 1)
    sub = lax.broadcasted_iota(jnp.int32, (8, 128), 0)

    def tile(g, w):
        return a[8 * g : 8 * g + 8, 128 * w : 128 * w + 128]

    def columns(rows, w, first):
        return [[column(r[w], first + q) for r in rows] for q in range(step)]

    now = [[tile(begin // 8 + g, w) for w in range(wide)] for g in range(per)]
    for first in range(begin, end, step):
        g0, w0, lane0 = first // 8, first // 128, first % 128
        inside = (lane >= lane0) & (lane < lane0 + step)
        more = first + step < size
        panel = [list(r) for r in now]
        c = columns(now, w0, lane0)
        if more:
            ahead = [[tile(g0 + per + i, w) for w in range(wide)] for i in range(per)]
            ahead_c = columns(ahead, w0, lane0)
        scale = [jnp.zeros((8, 128), jnp.float32)] * per
        pivot = row(c[0][0], 0)
        for i in range(per):
            unit = jnp.where(lane == sub + (lane0 + 8 * i), 1.0, 0.0)
            panel[i][w0] = jnp.where(inside, unit, panel[i][w0])
        for q in range(step):
            gq, sq = q // 8, q % 8
            here = sub == sq
            inv = 1.0 / pivot
            scale[gq] = jnp.where(here, inv, scale[gq])
            if q + 1 < step:
                gn, sn = (q + 1) // 8, (q + 1) % 8
                product = row(c[q][gn], sn) * row(c[q + 1][gq], sq)
                pivot = row(c[q + 1][gn], sn) - product * inv
            factor = [jnp.where(here, 0.0, c[q][i]) if i == gq else c[q][i] for i in range(per)]
            factor = [f * inv for f in factor]
            for p in range(q + 1, step):
                pivot_row = row(c[p][gq], sq)
                for i in range(per):
                    c[p][i] = c[p][i] - factor[i] * pivot_row
            for w in range(wide):
                pivot_row = row(panel[gq][w], sq)
                for i in range(per):
                    panel[i][w] = panel[i][w] - factor[i] * pivot_row
        done = [[panel[i][w] * scale[i] for w in range(wide)] for i in range(per)]
        lanes = lax.broadcasted_iota(jnp.int32, (step, size), 1)
        left = stack(now)
        left = thirds(jnp.where(lanes < first, -left, left))
        right = thirds(stack(done))
        pairs = ((0, 0), (0, 1), (1, 0), (0, 2), (1, 1), (2, 0))
        update = lax.dot_general(
            jnp.concatenate([left[i] for i, _ in pairs], axis=0),
            jnp.concatenate([right[i] for _, i in pairs], axis=0),
            (((0,), (0,)), ((), ())),
            preferred_element_type=jnp.float32,
        )
        if more:
            now = []
            for i in range(per):
                fresh = []
                for w in range(wide):
                    terms = [ahead_c[q][i] * row(done[q // 8][w], q % 8) for q in range(step)]
                    while len(terms) > 1:
                        terms = [x + y for x, y in zip(terms[::2], terms[1::2])]
                    spread = terms[0]
                    base = ahead[i][w]
                    base = jnp.where(inside, 0.0, base) if w == w0 else base
                    fresh.append(base - spread)
                now.append(fresh)
        for g in range(size // 8):
            for w in range(wide):
                if g0 <= g < g0 + per:
                    value = done[g - g0][w]
                elif more and g0 + per <= g < g0 + 2 * per:
                    value = now[g - g0 - per][w]
                else:
                    value = tile(g, w)
                    value = jnp.where(inside, 0.0, value) if w == w0 else value
                    value = value - update[8 * g : 8 * g + 8, 128 * w : 128 * w + 128]
                a[8 * g : 8 * g + 8, 128 * w : 128 * w + 128] = value


def first_kernel(nj, nk, height_b, flipped, blocks, where, held, c_cols, b_cols, *refs):
    owns, (kept, out, b_all) = refs[:nk], refs[nk:]
    rank = out.shape[1]

    def gram(x, contracted):
        dims = (((contracted,), (contracted,)), ((), ()))
        return lax.dot_general(x, x, dims, preferred_element_type=jnp.float32)

    for t in range(nk):
        part = owns[t][rank:, :].reshape(nj, height_b, owns[t].shape[1])
        if flipped:
            at = pl.multiple_of(wrap(where[1] - t, nk) * height_b, height_b)
            b_all[:, pl.ds(at, height_b), :] = part
        else:
            at = pl.multiple_of(wrap(where[1] - t, nk) * 128, 128)
            b_all[:, :, pl.ds(at, 128)] = part
    if flipped:
        gram_b = sum(gram(b_all[s], 1) for s in range(nj))
    else:
        gram_b = gram(b_all[...].reshape(nj * height_b, rank), 0)
    gram_c = sum(gram(own[:rank, :], 1) for own in owns)
    diagonal = lax.broadcasted_iota(jnp.int32, out.shape, 0) == lax.broadcasted_iota(
        jnp.int32, out.shape, 1
    )
    out[...] = gram_b * gram_c + jnp.where(diagonal, ridge_weight, 0.0)
    contract(held.at[0, : nj // 2], kept, c_cols[...], b_cols[...])
    invert(out, 0, blocks)


def rest_kernel(blocks, half_done, out):
    out[...] = half_done[...]
    invert(out, blocks, out.shape[0])


def solve_kernel(kept, received, inverse, out):
    mine = kept[0] + received[0]
    out[...] = jnp.dot(mine, inverse[...], precision=exact, preferred_element_type=jnp.float32)


def send(x, axis, n, s):
    return lax.ppermute(x, axis, shift(n, s))


def update(tensor, factor_b, factor_c):
    nj, nk = lax.axis_size("ja"), lax.axis_size("ka")
    where = jnp.stack([lax.axis_index("ja"), lax.axis_index("ka")]).astype(jnp.int32)
    rank = factor_b.shape[1] * nk
    flipped = factor_b.shape[1] % 128 != 0
    part_b = factor_b.T if flipped else factor_b
    height_b = part_b.shape[0]
    mine = jnp.concatenate([part_b, factor_c.T], axis=0)
    line = [mine] + [send(mine, "ja", nj, s) for s in range(1, nj)]
    b_parts = [mine] + [send(mine, "ka", nk, t) for t in range(1, nk)]
    held = fetch(where, tensor, nj, nk)
    away, own, c_cols, b_cols = contract_away(
        where, held, line, b_parts, height_b, flipped, rank
    )
    half = nj // 2
    turns = tuple(range(1, nk))
    owns = [own] + [send(own, "ka", nk, t) for t in turns]
    sent = contract_rows((0,), half, half, held, c_cols, b_cols)[0]
    for t in turns:
        sent = sent + send(away[t - 1], "ka", nk, t)
    received = lax.ppermute(sent, "ja", [(i, i ^ 1) for i in range(nj)])
    away = contract_rows(turns, 0, half, held, c_cols, b_cols)
    params = pltpu.CompilerParams(vmem_limit_bytes=20 * 2**20)
    cost = pl.CostEstimate(flops=5 * 10**9, bytes_accessed=2**20, transcendentals=0)
    square = jax.ShapeDtypeStruct((rank, rank), jnp.float32)
    blocks = rank // 64 * 16
    b_shape = (nj, rank, mine.shape[1]) if flipped else (nj, height_b, rank)
    kept, half_done = pl.pallas_call(
        functools.partial(first_kernel, nj, nk, height_b, flipped, blocks),
        out_shape=[jax.ShapeDtypeStruct(sent.shape, jnp.float32), square],
        in_specs=[smem] + [vmem] * (3 + nk),
        out_specs=[vmem] * 2,
        scratch_shapes=[pltpu.VMEM(b_shape, mine.dtype)],
        compiler_params=params,
        cost_estimate=cost,
    )(where, held, c_cols, b_cols, *owns)
    for t in turns:
        kept = kept + send(away[t - 1], "ka", nk, t)
    bit = 2
    while bit < nj:
        kept, sent = jnp.split(kept + received, 2, axis=0)
        received = lax.ppermute(sent, "ja", [(i, i ^ bit) for i in range(nj)])
        bit *= 2
    inverse = pl.pallas_call(
        functools.partial(rest_kernel, blocks),
        out_shape=square,
        in_specs=[vmem],
        out_specs=vmem,
        compiler_params=params,
        cost_estimate=cost,
    )(half_done)
    return pl.pallas_call(
        solve_kernel,
        out_shape=jax.ShapeDtypeStruct(kept.shape[1:], jnp.float32),
        in_specs=[vmem] * 3,
        out_specs=vmem,
        compiler_params=params,
        cost_estimate=pl.CostEstimate(flops=10**8, bytes_accessed=2**19, transcendentals=0),
    )(kept, received, inverse)


def solution(mesh):
    placed = (P("ia", "ja", "ka"), P("ja", "ka"), P("ka", "ja"))
    return jax.shard_map(
        update, mesh=mesh, in_specs=placed, out_specs=P(("ia", "ja", "ka"), None), check_vma=False
    )
```

```python
import functools

import jax
import jax.numpy as jnp
from jax import lax
from jax.experimental import pallas as pl
from jax.experimental.pallas import tpu as pltpu
from jax.sharding import PartitionSpec as P


ridge_weight = 0.1
vmem = pl.BlockSpec(memory_space=pltpu.VMEM)
smem = pl.BlockSpec(memory_space=pltpu.SMEM)
hbm = pl.BlockSpec(memory_space=pltpu.HBM)


def shift(n, s):
    return [(i, (i + s) % n) for i in range(n)]


def wrap(x, n):
    return lax.rem(x + n, n)


def owner(nk, where, t, u):
    return lax.bitwise_xor(where[0], u) * nk + wrap(where[1] + t, nk)


def halving_order(nj):
    order = [0]
    while len(order) < nj:
        order = [2 * u for u in order] + [2 * u + 1 for u in order]
    return order


def fetch_kernel(nj, nk, where, block, held, arrived):
    owned = held.shape[2]
    copies = []
    for t in range(nk):
        for slot, u in enumerate(halving_order(nj)):
            first = pl.multiple_of(owner(nk, where, t, u) * owned, owned)
            rows = block.at[pl.ds(first, owned)]
            copies.append(pltpu.make_async_copy(rows, held.at[t, slot], arrived.at[t, slot]))
    for copy in copies:
        copy.start()
    for copy in copies:
        copy.wait()


def fetch(where, tensor, nj, nk):
    rows, width_j, width_k = tensor.shape
    owned = rows // (nj * nk)
    return pl.pallas_call(
        functools.partial(fetch_kernel, nj, nk),
        out_shape=jax.ShapeDtypeStruct((nk, nj, owned, width_j, width_k), tensor.dtype),
        in_specs=[smem, hbm],
        out_specs=vmem,
        scratch_shapes=[pltpu.SemaphoreType.DMA((nk, nj))],
        compiler_params=pltpu.CompilerParams(vmem_limit_bytes=42 * 2**20),
        cost_estimate=pl.CostEstimate(
            flops=4 * 10**9, bytes_accessed=2 * rows * width_j * width_k, transcendentals=0
        ),
    )(where, tensor)


def contraction(held, out, c_wide, b_wide):
    count, owned = held.shape[0], held.shape[1]
    few = min(owned, 8)

    def piece(u, first):
        sums = []
        for i in range(first, first + few):
            inner = jnp.dot(held[u, i], c_wide, preferred_element_type=jnp.float32)
            sums.append(jnp.sum(inner * b_wide, axis=0, keepdims=True))
        out[u, first : first + few, :] = jnp.concatenate(sums, axis=0)

    return [
        functools.partial(piece, u, first) for u in range(count) for first in range(0, owned, few)
    ]


def contract(held, out, c_wide, b_wide):
    for piece in contraction(held, out, c_wide, b_wide):
        piece()


def share(pieces, turn, turns):
    for piece in pieces[len(pieces) * turn // turns : len(pieces) * (turn + 1) // turns]:
        piece()


def away_kernel(nj, nk, height_b, flipped, where, held, *refs):
    line, refs = refs[:nj], refs[nj:]
    b_parts, refs = refs[:nk], refs[nk:]
    out, own, c_cols, b_cols, b_rows = refs
    rank = c_cols.shape[1]
    width_c = line[0].shape[0] - height_b
    for s in range(nj):
        at = pl.multiple_of(wrap(where[0] - s, nj) * width_c, width_c)
        own[pl.ds(at, width_c), :] = line[s][height_b:, :]
        own[rank + s * height_b : rank + (s + 1) * height_b, :] = line[s][:height_b, :]
    for t in range(nk):
        if flipped:
            at = pl.multiple_of(wrap(where[1] - t, nk) * height_b, height_b)
            b_rows[pl.ds(at, height_b), :] = b_parts[t][:height_b, :]
        else:
            at = pl.multiple_of(wrap(where[1] - t, nk) * 128, 128)
            b_rows[:, pl.ds(at, 128)] = b_parts[t][:height_b, :]
    c_cols[...] = own[:rank, :].T
    b_cols[...] = (b_rows[...].T if flipped else b_rows[...]).astype(jnp.float32)
    for t in range(1, nk):
        contract(held.at[t, nj // 2 :], out.at[t - 1], c_cols[...], b_cols[...])


def rows_kernel(turns, begin, count, held, c_cols, b_cols, out):
    for slot, t in enumerate(turns):
        contract(held.at[t, begin : begin + count], out.at[slot], c_cols[...], b_cols[...])


def flops_of(rows, held, rank):
    return pl.CostEstimate(
        flops=2 * rows * held.shape[-2] * held.shape[-1] * rank,
        bytes_accessed=2**20,
        transcendentals=0,
    )


def contract_away(where, held, line, b_parts, height_b, flipped, rank):
    nk, nj, owned, width_j, width_k = held.shape
    width = line[0].shape[1]
    return pl.pallas_call(
        functools.partial(away_kernel, nj, nk, height_b, flipped),
        out_shape=[
            jax.ShapeDtypeStruct((nk - 1, nj // 2, owned, rank), jnp.float32),
            jax.ShapeDtypeStruct((rank + nj * height_b, width), held.dtype),
            jax.ShapeDtypeStruct((width_k, rank), held.dtype),
            jax.ShapeDtypeStruct((width_j, rank), jnp.float32),
        ],
        in_specs=[smem] + [vmem] * (1 + nj + nk),
        out_specs=[vmem] * 4,
        scratch_shapes=[pltpu.VMEM((rank, width_j) if flipped else (width_j, rank), held.dtype)],
        compiler_params=pltpu.CompilerParams(vmem_limit_bytes=20 * 2**20),
        cost_estimate=flops_of((nk - 1) * nj * owned // 2, held, rank),
    )(where, held, *line, *b_parts)


def contract_rows(turns, begin, count, held, c_cols, b_cols):
    owned, rank = held.shape[2], c_cols.shape[1]
    return pl.pallas_call(
        functools.partial(rows_kernel, turns, begin, count),
        out_shape=jax.ShapeDtypeStruct((len(turns), count, owned, rank), jnp.float32),
        in_specs=[vmem] * 3,
        out_specs=vmem,
        compiler_params=pltpu.CompilerParams(vmem_limit_bytes=20 * 2**20),
        cost_estimate=flops_of(len(turns) * count * owned, held, rank),
    )(held, c_cols, b_cols)


def column(x, q):
    return jnp.take_along_axis(x, jnp.full(x.shape, q, jnp.int32), axis=1)


def row(x, q):
    return jnp.broadcast_to(x[q : q + 1, :], x.shape)


def thirds(x):
    high = x.astype(jnp.bfloat16)
    x = x - high.astype(jnp.float32)
    middle = x.astype(jnp.bfloat16)
    return high, middle, (x - middle.astype(jnp.float32)).astype(jnp.bfloat16)


pairs = ((0, 0), (0, 1), (1, 0), (0, 2), (1, 1), (2, 0))


def stack(tiles):
    return jnp.concatenate([jnp.concatenate(r, axis=1) for r in tiles], axis=0)


def invert(a, begin, end, between=None, step=16):
    size = a.shape[0]
    wide, per = size // 128, step // 8
    lane = lax.broadcasted_iota(jnp.int32, (8, 128), 1)
    sub = lax.broadcasted_iota(jnp.int32, (8, 128), 0)

    def tile(g, w):
        return a[8 * g : 8 * g + 8, 128 * w : 128 * w + 128]

    def columns(rows, w, first):
        return [[column(r[w], first + q) for r in rows] for q in range(step)]

    now = [[tile(begin // 8 + g, w) for w in range(wide)] for g in range(per)]
    for first in range(begin, end, step):
        g0, w0, lane0 = first // 8, first // 128, first % 128
        inside = (lane >= lane0) & (lane < lane0 + step)
        more = first + step < size
        if between is not None:
            between((first - begin) // step)
        panel = [list(r) for r in now]
        c = columns(now, w0, lane0)
        if more:
            ahead = [[tile(g0 + per + i, w) for w in range(wide)] for i in range(per)]
            ahead_c = columns(ahead, w0, lane0)
        scale = [jnp.zeros((8, 128), jnp.float32)] * per
        pivot = row(c[0][0], 0)
        for i in range(per):
            unit = jnp.where(lane == sub + (lane0 + 8 * i), 1.0, 0.0)
            panel[i][w0] = jnp.where(inside, unit, panel[i][w0])
        for q in range(step):
            gq, sq = q // 8, q % 8
            here = sub == sq
            inv = 1.0 / pivot
            scale[gq] = jnp.where(here, inv, scale[gq])
            if q + 1 < step:
                gn, sn = (q + 1) // 8, (q + 1) % 8
                product = row(c[q][gn], sn) * row(c[q + 1][gq], sq)
                pivot = row(c[q + 1][gn], sn) - product * inv
            factor = [jnp.where(here, 0.0, c[q][i]) if i == gq else c[q][i] for i in range(per)]
            factor = [f * inv for f in factor]
            for p in range(q + 1, step):
                pivot_row = row(c[p][gq], sq)
                for i in range(per):
                    c[p][i] = c[p][i] - factor[i] * pivot_row
            for w in range(wide):
                pivot_row = row(panel[gq][w], sq)
                for i in range(per):
                    panel[i][w] = panel[i][w] - factor[i] * pivot_row
        done = [[panel[i][w] * scale[i] for w in range(wide)] for i in range(per)]
        lanes = lax.broadcasted_iota(jnp.int32, (step, size), 1)
        left = stack(now)
        left = thirds(jnp.where(lanes < first, -left, left))
        right = thirds(stack(done))
        update = lax.dot_general(
            jnp.concatenate([left[i] for i, _ in pairs], axis=0),
            jnp.concatenate([right[i] for _, i in pairs], axis=0),
            (((0,), (0,)), ((), ())),
            preferred_element_type=jnp.float32,
        )
        if more:
            now = []
            for i in range(per):
                fresh = []
                for w in range(wide):
                    terms = [ahead_c[q][i] * row(done[q // 8][w], q % 8) for q in range(step)]
                    while len(terms) > 1:
                        terms = [x + y for x, y in zip(terms[::2], terms[1::2])]
                    spread = terms[0]
                    base = ahead[i][w]
                    base = jnp.where(inside, 0.0, base) if w == w0 else base
                    fresh.append(base - spread)
                now.append(fresh)
        for g in range(size // 8):
            for w in range(wide):
                if g0 <= g < g0 + per:
                    value = done[g - g0][w]
                elif more and g0 + per <= g < g0 + 2 * per:
                    value = now[g - g0 - per][w]
                else:
                    value = tile(g, w)
                    value = jnp.where(inside, 0.0, value) if w == w0 else value
                    value = value - update[8 * g : 8 * g + 8, 128 * w : 128 * w + 128]
                a[8 * g : 8 * g + 8, 128 * w : 128 * w + 128] = value


def first_kernel(nj, nk, height_b, flipped, blocks, where, held, c_cols, b_cols, *refs):
    owns, (away, out, b_all) = refs[:nk], refs[nk:]
    rank = out.shape[1]
    pieces = []
    for t in range(1, nk):
        pieces += contraction(held.at[t, : nj // 2], away.at[t - 1], c_cols[...], b_cols[...])
    turns = blocks // 16 + 1

    def gram(x, contracted):
        dims = (((contracted,), (contracted,)), ((), ()))
        return lax.dot_general(x, x, dims, preferred_element_type=jnp.float32)

    for t in range(nk):
        part = owns[t][rank:, :].reshape(nj, height_b, owns[t].shape[1])
        if flipped:
            at = pl.multiple_of(wrap(where[1] - t, nk) * height_b, height_b)
            b_all[:, pl.ds(at, height_b), :] = part
        else:
            at = pl.multiple_of(wrap(where[1] - t, nk) * 128, 128)
            b_all[:, :, pl.ds(at, 128)] = part
    if flipped:
        gram_b = sum(gram(b_all[s], 1) for s in range(nj))
    else:
        gram_b = gram(b_all[...].reshape(nj * height_b, rank), 0)
    gram_c = sum(gram(own[:rank, :], 1) for own in owns)
    share(pieces, 0, turns)
    diagonal = lax.broadcasted_iota(jnp.int32, out.shape, 0) == lax.broadcasted_iota(
        jnp.int32, out.shape, 1
    )
    out[...] = gram_b * gram_c + jnp.where(diagonal, ridge_weight, 0.0)
    invert(out, 0, blocks, lambda turn: share(pieces, turn + 1, turns))


def middle_kernel(begin, end, held, c_cols, b_cols, started, kept, out):
    out[...] = started[...]
    half = kept.shape[0]
    pieces = contraction(held.at[0, :half], kept, c_cols[...], b_cols[...])
    turns = (end - begin) // 16
    invert(out, begin, end, lambda turn: share(pieces, turn, turns))


def rest_kernel(blocks, half_done, out):
    out[...] = half_done[...]
    invert(out, blocks, out.shape[0])


def solve_kernel(kept, received, inverse, out):
    left, right = thirds(kept[0] + received[0]), thirds(inverse[...])
    out[...] = jnp.dot(
        jnp.concatenate([left[i] for i, _ in pairs], axis=1),
        jnp.concatenate([right[i] for _, i in pairs], axis=0),
        preferred_element_type=jnp.float32,
    )


def send(x, axis, n, s):
    return lax.ppermute(x, axis, shift(n, s))


def update(tensor, factor_b, factor_c):
    nj, nk = lax.axis_size("ja"), lax.axis_size("ka")
    where = jnp.stack([lax.axis_index("ja"), lax.axis_index("ka")]).astype(jnp.int32)
    rank = factor_b.shape[1] * nk
    flipped = factor_b.shape[1] % 128 != 0
    part_b = factor_b.T if flipped else factor_b
    height_b = part_b.shape[0]
    mine = jnp.concatenate([part_b, factor_c.T], axis=0)
    line = [mine] + [send(mine, "ja", nj, s) for s in range(1, nj)]
    b_parts = [mine] + [send(mine, "ka", nk, t) for t in range(1, nk)]
    held = fetch(where, tensor, nj, nk)
    away, own, c_cols, b_cols = contract_away(
        where, held, line, b_parts, height_b, flipped, rank
    )
    half = nj // 2
    turns = tuple(range(1, nk))
    owns = [own] + [send(own, "ka", nk, t) for t in turns]
    sent = contract_rows((0,), half, half, held, c_cols, b_cols)[0]
    for t in turns:
        sent = sent + send(away[t - 1], "ka", nk, t)
    received = lax.ppermute(sent, "ja", [(i, i ^ 1) for i in range(nj)])
    params = pltpu.CompilerParams(vmem_limit_bytes=20 * 2**20)
    cost = pl.CostEstimate(flops=5 * 10**9, bytes_accessed=2**20, transcendentals=0)
    square = jax.ShapeDtypeStruct((rank, rank), jnp.float32)
    first, middle = rank // 128 * 16, rank // 256 * 80
    b_shape = (nj, rank, mine.shape[1]) if flipped else (nj, height_b, rank)
    away, started = pl.pallas_call(
        functools.partial(first_kernel, nj, nk, height_b, flipped, first),
        out_shape=[jax.ShapeDtypeStruct(away.shape, jnp.float32), square],
        in_specs=[smem] + [vmem] * (3 + nk),
        out_specs=[vmem] * 2,
        scratch_shapes=[pltpu.VMEM(b_shape, mine.dtype)],
        compiler_params=params,
        cost_estimate=cost,
    )(where, held, c_cols, b_cols, *owns)
    kept, half_done = pl.pallas_call(
        functools.partial(middle_kernel, first, middle),
        out_shape=[jax.ShapeDtypeStruct(sent.shape, jnp.float32), square],
        in_specs=[vmem] * 4,
        out_specs=[vmem] * 2,
        compiler_params=params,
        cost_estimate=cost,
    )(held, c_cols, b_cols, started)
    for t in turns:
        kept = kept + send(away[t - 1], "ka", nk, t)
    bit = 2
    while bit < nj:
        kept, sent = jnp.split(kept + received, 2, axis=0)
        received = lax.ppermute(sent, "ja", [(i, i ^ bit) for i in range(nj)])
        bit *= 2
    inverse = pl.pallas_call(
        functools.partial(rest_kernel, middle),
        out_shape=square,
        in_specs=[vmem],
        out_specs=vmem,
        compiler_params=params,
        cost_estimate=cost,
    )(half_done)
    return pl.pallas_call(
        solve_kernel,
        out_shape=jax.ShapeDtypeStruct(kept.shape[1:], jnp.float32),
        in_specs=[vmem] * 3,
        out_specs=vmem,
        compiler_params=params,
        cost_estimate=pl.CostEstimate(flops=10**8, bytes_accessed=2**19, transcendentals=0),
    )(kept, received, inverse)


def solution(mesh):
    placed = (P("ia", "ja", "ka"), P("ja", "ka"), P("ka", "ja"))
    return jax.shard_map(
        update, mesh=mesh, in_specs=placed, out_specs=P(("ia", "ja", "ka"), None), check_vma=False
    )
```

```python
import functools

import jax
import jax.numpy as jnp
from jax import lax
from jax.experimental import pallas as pl
from jax.experimental.pallas import tpu as pltpu
from jax.sharding import PartitionSpec as P


ridge_weight = 0.1
vmem = pl.BlockSpec(memory_space=pltpu.VMEM)
smem = pl.BlockSpec(memory_space=pltpu.SMEM)
hbm = pl.BlockSpec(memory_space=pltpu.HBM)


def shift(n, s):
    return [(i, (i + s) % n) for i in range(n)]


def wrap(x, n):
    return lax.rem(x + n, n)


def owner(nk, where, t, u):
    return lax.bitwise_xor(where[0], u) * nk + wrap(where[1] + t, nk)


def halving_order(nj):
    order = [0]
    while len(order) < nj:
        order = [2 * u for u in order] + [2 * u + 1 for u in order]
    return order


def owner_rows(nj, nk, where, block, t, slot, owned):
    to = owner(nk, where, t, halving_order(nj)[slot])
    return block.at[pl.ds(pl.multiple_of(to * owned, owned), owned)]


def fetch_kernel(nj, nk, where, block, away_held, sent_held, arrived):
    owned, half = sent_held.shape[1], nj // 2
    targets = [(t, slot, away_held.at[t - 1, slot]) for t in range(1, nk) for slot in range(nj)]
    targets += [(0, slot, sent_held.at[slot - half]) for slot in range(half, nj)]
    copies = []
    for i, (t, slot, target) in enumerate(targets):
        rows = owner_rows(nj, nk, where, block, t, slot, owned)
        copies.append(pltpu.make_async_copy(rows, target, arrived.at[i]))
    for copy in copies:
        copy.start()
    for copy in copies:
        copy.wait()


def fetch(where, tensor, nj, nk):
    rows, width_j, width_k = tensor.shape
    owned = rows // (nj * nk)
    return pl.pallas_call(
        functools.partial(fetch_kernel, nj, nk),
        out_shape=[
            jax.ShapeDtypeStruct((nk - 1, nj, owned, width_j, width_k), tensor.dtype),
            jax.ShapeDtypeStruct((nj // 2, owned, width_j, width_k), tensor.dtype),
        ],
        in_specs=[smem, hbm],
        out_specs=[vmem] * 2,
        scratch_shapes=[pltpu.SemaphoreType.DMA(((nk - 1) * nj + nj // 2,))],
        compiler_params=pltpu.CompilerParams(vmem_limit_bytes=44 * 2**20),
        cost_estimate=pl.CostEstimate(
            flops=4 * 10**9, bytes_accessed=2 * rows * width_j * width_k, transcendentals=0
        ),
    )(where, tensor)


def contraction(held, out, c_wide, b_wide):
    count, owned = held.shape[0], held.shape[1]
    few = min(owned, 8)

    def piece(u, first):
        sums = []
        for i in range(first, first + few):
            inner = jnp.dot(held[u, i], c_wide, preferred_element_type=jnp.float32)
            sums.append(jnp.sum(inner * b_wide, axis=0, keepdims=True))
        out[u, first : first + few, :] = jnp.concatenate(sums, axis=0)

    return [
        functools.partial(piece, u, first) for u in range(count) for first in range(0, owned, few)
    ]


def contract(held, out, c_wide, b_wide):
    for piece in contraction(held, out, c_wide, b_wide):
        piece()


def share(pieces, turn, turns):
    for piece in pieces[len(pieces) * turn // turns : len(pieces) * (turn + 1) // turns]:
        piece()


def away_kernel(nj, nk, height_b, flipped, where, block, held, *refs):
    line, refs = refs[:nj], refs[nj:]
    b_parts, refs = refs[:nk], refs[nk:]
    out, own, c_cols, b_cols, kept_held, b_rows, arrived = refs
    rank, owned = c_cols.shape[1], kept_held.shape[1]
    order = halving_order(nj)

    def load(slot):
        to = wrap(where[1], nk)
        u = sum(jnp.where(slot == i, order[i], 0) for i in range(nj // 2))
        to = lax.bitwise_xor(where[0], u) * nk + to
        rows = block.at[pl.ds(pl.multiple_of(to * owned, owned), owned)]
        return pltpu.make_async_copy(rows, kept_held.at[slot], arrived.at[slot])

    def begin(slot, _):
        load(slot).start()
        return 0

    def finish(slot, _):
        load(slot).wait()
        return 0

    lax.fori_loop(0, nj // 2, begin, 0)
    width_c = line[0].shape[0] - height_b
    for s in range(nj):
        at = pl.multiple_of(wrap(where[0] - s, nj) * width_c, width_c)
        own[pl.ds(at, width_c), :] = line[s][height_b:, :]
        own[rank + s * height_b : rank + (s + 1) * height_b, :] = line[s][:height_b, :]
    for t in range(nk):
        if flipped:
            at = pl.multiple_of(wrap(where[1] - t, nk) * height_b, height_b)
            b_rows[pl.ds(at, height_b), :] = b_parts[t][:height_b, :]
        else:
            at = pl.multiple_of(wrap(where[1] - t, nk) * 128, 128)
            b_rows[:, pl.ds(at, 128)] = b_parts[t][:height_b, :]
    c_cols[...] = own[:rank, :].T
    b_cols[...] = (b_rows[...].T if flipped else b_rows[...]).astype(jnp.float32)
    for t in range(1, nk):
        contract(held.at[t - 1, nj // 2 :], out.at[t - 1], c_cols[...], b_cols[...])
    lax.fori_loop(0, nj // 2, finish, 0)


def rows_kernel(held, c_cols, b_cols, out):
    contract(held, out, c_cols[...], b_cols[...])


def flops_of(rows, held, rank):
    return pl.CostEstimate(
        flops=2 * rows * held.shape[-2] * held.shape[-1] * rank,
        bytes_accessed=2**20,
        transcendentals=0,
    )


def contract_away(where, tensor, held, line, b_parts, height_b, flipped, rank):
    _, nj, owned, width_j, width_k = held.shape
    nk = len(b_parts)
    width = line[0].shape[1]
    return pl.pallas_call(
        functools.partial(away_kernel, nj, nk, height_b, flipped),
        out_shape=[
            jax.ShapeDtypeStruct((nk - 1, nj // 2, owned, rank), jnp.float32),
            jax.ShapeDtypeStruct((rank + nj * height_b, width), held.dtype),
            jax.ShapeDtypeStruct((width_k, rank), held.dtype),
            jax.ShapeDtypeStruct((width_j, rank), jnp.float32),
            jax.ShapeDtypeStruct((nj // 2, owned, width_j, width_k), held.dtype),
        ],
        in_specs=[smem, hbm] + [vmem] * (1 + nj + nk),
        out_specs=[vmem] * 5,
        scratch_shapes=[
            pltpu.VMEM((rank, width_j) if flipped else (width_j, rank), held.dtype),
            pltpu.SemaphoreType.DMA((nj // 2,)),
        ],
        compiler_params=pltpu.CompilerParams(vmem_limit_bytes=44 * 2**20),
        cost_estimate=flops_of((nk - 1) * nj * owned // 2, held, rank),
    )(where, tensor, held, *line, *b_parts)


def contract_rows(held, c_cols, b_cols):
    count, owned = held.shape[:2]
    rank = c_cols.shape[1]
    return pl.pallas_call(
        rows_kernel,
        out_shape=jax.ShapeDtypeStruct((count, owned, rank), jnp.float32),
        in_specs=[vmem] * 3,
        out_specs=vmem,
        compiler_params=pltpu.CompilerParams(vmem_limit_bytes=20 * 2**20),
        cost_estimate=flops_of(count * owned, held, rank),
    )(held, c_cols, b_cols)


def column(x, q):
    return jnp.take_along_axis(x, jnp.full(x.shape, q, jnp.int32), axis=1)


def row(x, q):
    return jnp.broadcast_to(x[q : q + 1, :], x.shape)


def thirds(x):
    high = x.astype(jnp.bfloat16)
    x = x - high.astype(jnp.float32)
    middle = x.astype(jnp.bfloat16)
    return high, middle, (x - middle.astype(jnp.float32)).astype(jnp.bfloat16)


pairs = ((0, 0), (0, 1), (1, 0), (0, 2), (1, 1), (2, 0))


def stack(tiles):
    return jnp.concatenate([jnp.concatenate(r, axis=1) for r in tiles], axis=0)


def invert(a, begin, end, between=None, step=16):
    size = a.shape[0]
    wide, per = size // 128, step // 8
    lane = lax.broadcasted_iota(jnp.int32, (8, 128), 1)
    sub = lax.broadcasted_iota(jnp.int32, (8, 128), 0)

    def tile(g, w):
        return a[8 * g : 8 * g + 8, 128 * w : 128 * w + 128]

    def columns(rows, w, first):
        return [[column(r[w], first + q) for r in rows] for q in range(step)]

    now = [[tile(begin // 8 + g, w) for w in range(wide)] for g in range(per)]
    for first in range(begin, end, step):
        g0, w0, lane0 = first // 8, first // 128, first % 128
        inside = (lane >= lane0) & (lane < lane0 + step)
        more = first + step < size
        if between is not None:
            between((first - begin) // step)
        panel = [list(r) for r in now]
        c = columns(now, w0, lane0)
        if more:
            ahead = [[tile(g0 + per + i, w) for w in range(wide)] for i in range(per)]
            ahead_c = columns(ahead, w0, lane0)
        scale = [jnp.zeros((8, 128), jnp.float32)] * per
        pivot = row(c[0][0], 0)
        for i in range(per):
            unit = jnp.where(lane == sub + (lane0 + 8 * i), 1.0, 0.0)
            panel[i][w0] = jnp.where(inside, unit, panel[i][w0])
        for q in range(step):
            gq, sq = q // 8, q % 8
            here = sub == sq
            inv = 1.0 / pivot
            scale[gq] = jnp.where(here, inv, scale[gq])
            if q + 1 < step:
                gn, sn = (q + 1) // 8, (q + 1) % 8
                product = row(c[q][gn], sn) * row(c[q + 1][gq], sq)
                pivot = row(c[q + 1][gn], sn) - product * inv
            factor = [jnp.where(here, 0.0, c[q][i]) if i == gq else c[q][i] for i in range(per)]
            factor = [f * inv for f in factor]
            for p in range(q + 1, step):
                pivot_row = row(c[p][gq], sq)
                for i in range(per):
                    c[p][i] = c[p][i] - factor[i] * pivot_row
            for w in range(wide):
                pivot_row = row(panel[gq][w], sq)
                for i in range(per):
                    panel[i][w] = panel[i][w] - factor[i] * pivot_row
        done = [[panel[i][w] * scale[i] for w in range(wide)] for i in range(per)]
        lanes = lax.broadcasted_iota(jnp.int32, (step, size), 1)
        left = stack(now)
        left = thirds(jnp.where(lanes < first, -left, left))
        right = thirds(stack(done))
        update = lax.dot_general(
            jnp.concatenate([left[i] for i, _ in pairs], axis=0),
            jnp.concatenate([right[i] for _, i in pairs], axis=0),
            (((0,), (0,)), ((), ())),
            preferred_element_type=jnp.float32,
        )
        if more:
            now = []
            for i in range(per):
                fresh = []
                for w in range(wide):
                    terms = [ahead_c[q][i] * row(done[q // 8][w], q % 8) for q in range(step)]
                    while len(terms) > 1:
                        terms = [x + y for x, y in zip(terms[::2], terms[1::2])]
                    spread = terms[0]
                    base = ahead[i][w]
                    base = jnp.where(inside, 0.0, base) if w == w0 else base
                    fresh.append(base - spread)
                now.append(fresh)
        for g in range(size // 8):
            for w in range(wide):
                if g0 <= g < g0 + per:
                    value = done[g - g0][w]
                elif more and g0 + per <= g < g0 + 2 * per:
                    value = now[g - g0 - per][w]
                else:
                    value = tile(g, w)
                    value = jnp.where(inside, 0.0, value) if w == w0 else value
                    value = value - update[8 * g : 8 * g + 8, 128 * w : 128 * w + 128]
                a[8 * g : 8 * g + 8, 128 * w : 128 * w + 128] = value


def first_kernel(nj, nk, height_b, flipped, blocks, where, held, c_cols, b_cols, *refs):
    owns, (away, out, b_all) = refs[:nk], refs[nk:]
    rank = out.shape[1]
    pieces = []
    for t in range(1, nk):
        pieces += contraction(held.at[t - 1, : nj // 2], away.at[t - 1], c_cols[...], b_cols[...])
    turns = blocks // 16 + 1

    def gram(x, contracted):
        dims = (((contracted,), (contracted,)), ((), ()))
        return lax.dot_general(x, x, dims, preferred_element_type=jnp.float32)

    for t in range(nk):
        part = owns[t][rank:, :].reshape(nj, height_b, owns[t].shape[1])
        if flipped:
            at = pl.multiple_of(wrap(where[1] - t, nk) * height_b, height_b)
            b_all[:, pl.ds(at, height_b), :] = part
        else:
            at = pl.multiple_of(wrap(where[1] - t, nk) * 128, 128)
            b_all[:, :, pl.ds(at, 128)] = part
    if flipped:
        gram_b = sum(gram(b_all[s], 1) for s in range(nj))
    else:
        gram_b = gram(b_all[...].reshape(nj * height_b, rank), 0)
    gram_c = sum(gram(own[:rank, :], 1) for own in owns)
    share(pieces, 0, turns)
    diagonal = lax.broadcasted_iota(jnp.int32, out.shape, 0) == lax.broadcasted_iota(
        jnp.int32, out.shape, 1
    )
    out[...] = gram_b * gram_c + jnp.where(diagonal, ridge_weight, 0.0)
    invert(out, 0, blocks, lambda turn: share(pieces, turn + 1, turns))


def middle_kernel(begin, end, held, c_cols, b_cols, started, kept, out):
    out[...] = started[...]
    pieces = contraction(held, kept, c_cols[...], b_cols[...])
    turns = (end - begin) // 16
    invert(out, begin, end, lambda turn: share(pieces, turn, turns))


def rest_kernel(blocks, half_done, out):
    out[...] = half_done[...]
    invert(out, blocks, out.shape[0])


def solve_kernel(kept, received, inverse, out):
    left, right = thirds(kept[0] + received[0]), thirds(inverse[...])
    out[...] = jnp.dot(
        jnp.concatenate([left[i] for i, _ in pairs], axis=1),
        jnp.concatenate([right[i] for _, i in pairs], axis=0),
        preferred_element_type=jnp.float32,
    )


def send(x, axis, n, s):
    return lax.ppermute(x, axis, shift(n, s))


def update(tensor, factor_b, factor_c):
    nj, nk = lax.axis_size("ja"), lax.axis_size("ka")
    where = jnp.stack([lax.axis_index("ja"), lax.axis_index("ka")]).astype(jnp.int32)
    rank = factor_b.shape[1] * nk
    flipped = factor_b.shape[1] % 128 != 0
    part_b = factor_b.T if flipped else factor_b
    height_b = part_b.shape[0]
    mine = jnp.concatenate([part_b, factor_c.T], axis=0)
    line = [mine] + [send(mine, "ja", nj, s) for s in range(1, nj)]
    b_parts = [mine] + [send(mine, "ka", nk, t) for t in range(1, nk)]
    away_held, sent_held = fetch(where, tensor, nj, nk)
    away, own, c_cols, b_cols, kept_held = contract_away(
        where, tensor, away_held, line, b_parts, height_b, flipped, rank
    )
    turns = tuple(range(1, nk))
    owns = [own] + [send(own, "ka", nk, t) for t in turns]
    sent = contract_rows(sent_held, c_cols, b_cols)
    for t in turns:
        sent = sent + send(away[t - 1], "ka", nk, t)
    received = lax.ppermute(sent, "ja", [(i, i ^ 1) for i in range(nj)])
    params = pltpu.CompilerParams(vmem_limit_bytes=20 * 2**20)
    cost = pl.CostEstimate(flops=5 * 10**9, bytes_accessed=2**20, transcendentals=0)
    square = jax.ShapeDtypeStruct((rank, rank), jnp.float32)
    first, middle = rank // 128 * 16, rank // 256 * 80
    b_shape = (nj, rank, mine.shape[1]) if flipped else (nj, height_b, rank)
    away, started = pl.pallas_call(
        functools.partial(first_kernel, nj, nk, height_b, flipped, first),
        out_shape=[jax.ShapeDtypeStruct(away.shape, jnp.float32), square],
        in_specs=[smem] + [vmem] * (3 + nk),
        out_specs=[vmem] * 2,
        scratch_shapes=[pltpu.VMEM(b_shape, mine.dtype)],
        compiler_params=params,
        cost_estimate=cost,
    )(where, away_held, c_cols, b_cols, *owns)
    kept, half_done = pl.pallas_call(
        functools.partial(middle_kernel, first, middle),
        out_shape=[jax.ShapeDtypeStruct(sent.shape, jnp.float32), square],
        in_specs=[vmem] * 4,
        out_specs=[vmem] * 2,
        compiler_params=params,
        cost_estimate=cost,
    )(kept_held, c_cols, b_cols, started)
    for t in turns:
        kept = kept + send(away[t - 1], "ka", nk, t)
    bit = 2
    while bit < nj:
        kept, sent = jnp.split(kept + received, 2, axis=0)
        received = lax.ppermute(sent, "ja", [(i, i ^ bit) for i in range(nj)])
        bit *= 2
    inverse = pl.pallas_call(
        functools.partial(rest_kernel, middle),
        out_shape=square,
        in_specs=[vmem],
        out_specs=vmem,
        compiler_params=params,
        cost_estimate=cost,
    )(half_done)
    return pl.pallas_call(
        solve_kernel,
        out_shape=jax.ShapeDtypeStruct(kept.shape[1:], jnp.float32),
        in_specs=[vmem] * 3,
        out_specs=vmem,
        compiler_params=params,
        cost_estimate=pl.CostEstimate(flops=10**8, bytes_accessed=2**19, transcendentals=0),
    )(kept, received, inverse)


def solution(mesh):
    placed = (P("ia", "ja", "ka"), P("ja", "ka"), P("ka", "ja"))
    return jax.shard_map(
        update, mesh=mesh, in_specs=placed, out_specs=P(("ia", "ja", "ka"), None), check_vma=False
    )
```

```python
import functools

import jax
import jax.numpy as jnp
from jax import lax
from jax.experimental import pallas as pl
from jax.experimental.pallas import tpu as pltpu
from jax.sharding import PartitionSpec as P


ridge_weight = 0.1
vmem = pl.BlockSpec(memory_space=pltpu.VMEM)
hbm = pl.BlockSpec(memory_space=pltpu.HBM)


def shift(n, s):
    return [(i, (i + s) % n) for i in range(n)]


def wrap(x, n):
    return lax.rem(x + n, n)


def owner(nk, where, t, u):
    return lax.bitwise_xor(where[0], u) * nk + wrap(where[1] + t, nk)


def halving_order(nj):
    order = [0]
    while len(order) < nj:
        order = [2 * u for u in order] + [2 * u + 1 for u in order]
    return order


def place():
    return lax.axis_index("ja"), lax.axis_index("ka")


def fetch_kernel(nj, nk, block, held, arrived):
    where = place()
    owned = held.shape[2]
    copies = []
    for t in range(nk):
        for slot, u in enumerate(halving_order(nj)):
            first = pl.multiple_of(owner(nk, where, t, u) * owned, owned)
            rows = block.at[pl.ds(first, owned)]
            copies.append(pltpu.make_async_copy(rows, held.at[t, slot], arrived.at[t, slot]))
    for copy in copies:
        copy.start()
    for copy in copies:
        copy.wait()


def fetch(tensor, nj, nk):
    rows, width_j, width_k = tensor.shape
    owned = rows // (nj * nk)
    return pl.pallas_call(
        functools.partial(fetch_kernel, nj, nk),
        out_shape=jax.ShapeDtypeStruct((nk, nj, owned, width_j, width_k), tensor.dtype),
        in_specs=[hbm],
        out_specs=vmem,
        scratch_shapes=[pltpu.SemaphoreType.DMA((nk, nj))],
        compiler_params=pltpu.CompilerParams(vmem_limit_bytes=42 * 2**20),
        cost_estimate=pl.CostEstimate(
            flops=4 * 10**9, bytes_accessed=2 * rows * width_j * width_k, transcendentals=0
        ),
    )(tensor)


def contraction(held, out, c_wide, b_wide):
    count, owned = held.shape[0], held.shape[1]
    few = min(owned, 8)

    def piece(u, first):
        sums = []
        for i in range(first, first + few):
            inner = jnp.dot(held[u, i], c_wide, preferred_element_type=jnp.float32)
            sums.append(jnp.sum(inner * b_wide, axis=0, keepdims=True))
        out[u, first : first + few, :] = jnp.concatenate(sums, axis=0)

    return [
        functools.partial(piece, u, first) for u in range(count) for first in range(0, owned, few)
    ]


def contract(held, out, c_wide, b_wide):
    for piece in contraction(held, out, c_wide, b_wide):
        piece()


def share(pieces, turn, turns):
    for piece in pieces[len(pieces) * turn // turns : len(pieces) * (turn + 1) // turns]:
        piece()


def away_kernel(nj, nk, height_b, flipped, held, *refs):
    where = place()
    line, refs = refs[:nj], refs[nj:]
    b_parts, refs = refs[:nk], refs[nk:]
    out, own, c_cols, b_cols, b_rows = refs
    rank = c_cols.shape[1]
    width_c = line[0].shape[0] - height_b
    for s in range(nj):
        at = pl.multiple_of(wrap(where[0] - s, nj) * width_c, width_c)
        own[pl.ds(at, width_c), :] = line[s][height_b:, :]
        own[rank + s * height_b : rank + (s + 1) * height_b, :] = line[s][:height_b, :]
    for t in range(nk):
        if flipped:
            at = pl.multiple_of(wrap(where[1] - t, nk) * height_b, height_b)
            b_rows[pl.ds(at, height_b), :] = b_parts[t][:height_b, :]
        else:
            at = pl.multiple_of(wrap(where[1] - t, nk) * 128, 128)
            b_rows[:, pl.ds(at, 128)] = b_parts[t][:height_b, :]
    c_cols[...] = own[:rank, :].T
    b_cols[...] = (b_rows[...].T if flipped else b_rows[...]).astype(jnp.float32)
    for t in range(1, nk):
        contract(held.at[t, nj // 2 :], out.at[t - 1], c_cols[...], b_cols[...])


def rows_kernel(turns, begin, count, held, c_cols, b_cols, out):
    for slot, t in enumerate(turns):
        contract(held.at[t, begin : begin + count], out.at[slot], c_cols[...], b_cols[...])


def flops_of(rows, held, rank):
    return pl.CostEstimate(
        flops=2 * rows * held.shape[-2] * held.shape[-1] * rank,
        bytes_accessed=2**20,
        transcendentals=0,
    )


def contract_away(held, line, b_parts, height_b, flipped, rank):
    nk, nj, owned, width_j, width_k = held.shape
    width = line[0].shape[1]
    return pl.pallas_call(
        functools.partial(away_kernel, nj, nk, height_b, flipped),
        out_shape=[
            jax.ShapeDtypeStruct((nk - 1, nj // 2, owned, rank), jnp.float32),
            jax.ShapeDtypeStruct((rank + nj * height_b, width), held.dtype),
            jax.ShapeDtypeStruct((width_k, rank), held.dtype),
            jax.ShapeDtypeStruct((width_j, rank), jnp.float32),
        ],
        in_specs=[vmem] * (1 + nj + nk),
        out_specs=[vmem] * 4,
        scratch_shapes=[pltpu.VMEM((rank, width_j) if flipped else (width_j, rank), held.dtype)],
        compiler_params=pltpu.CompilerParams(vmem_limit_bytes=20 * 2**20),
        cost_estimate=flops_of((nk - 1) * nj * owned // 2, held, rank),
    )(held, *line, *b_parts)


def contract_rows(turns, begin, count, held, c_cols, b_cols):
    owned, rank = held.shape[2], c_cols.shape[1]
    return pl.pallas_call(
        functools.partial(rows_kernel, turns, begin, count),
        out_shape=jax.ShapeDtypeStruct((len(turns), count, owned, rank), jnp.float32),
        in_specs=[vmem] * 3,
        out_specs=vmem,
        compiler_params=pltpu.CompilerParams(vmem_limit_bytes=20 * 2**20),
        cost_estimate=flops_of(len(turns) * count * owned, held, rank),
    )(held, c_cols, b_cols)


def column(x, q):
    return jnp.take_along_axis(x, jnp.full(x.shape, q, jnp.int32), axis=1)


def row(x, q):
    return jnp.broadcast_to(x[q : q + 1, :], x.shape)


def thirds(x):
    high = x.astype(jnp.bfloat16)
    x = x - high.astype(jnp.float32)
    middle = x.astype(jnp.bfloat16)
    return high, middle, (x - middle.astype(jnp.float32)).astype(jnp.bfloat16)


pairs = ((0, 0), (0, 1), (1, 0), (0, 2), (1, 1), (2, 0))


def stack(tiles):
    return jnp.concatenate([jnp.concatenate(r, axis=1) for r in tiles], axis=0)


def invert(a, begin, end, between=None, step=16):
    size = a.shape[0]
    wide, per = size // 128, step // 8
    lane = lax.broadcasted_iota(jnp.int32, (8, 128), 1)
    sub = lax.broadcasted_iota(jnp.int32, (8, 128), 0)

    def tile(g, w):
        return a[8 * g : 8 * g + 8, 128 * w : 128 * w + 128]

    def columns(rows, w, first):
        return [[column(r[w], first + q) for r in rows] for q in range(step)]

    now = [[tile(begin // 8 + g, w) for w in range(wide)] for g in range(per)]
    for first in range(begin, end, step):
        g0, w0, lane0 = first // 8, first // 128, first % 128
        inside = (lane >= lane0) & (lane < lane0 + step)
        more = first + step < size
        if between is not None:
            between((first - begin) // step)
        panel = [list(r) for r in now]
        c = columns(now, w0, lane0)
        if more:
            ahead = [[tile(g0 + per + i, w) for w in range(wide)] for i in range(per)]
            ahead_c = columns(ahead, w0, lane0)
        scale = [jnp.zeros((8, 128), jnp.float32)] * per
        pivot = row(c[0][0], 0)
        for i in range(per):
            unit = jnp.where(lane == sub + (lane0 + 8 * i), 1.0, 0.0)
            panel[i][w0] = jnp.where(inside, unit, panel[i][w0])
        for q in range(step):
            gq, sq = q // 8, q % 8
            here = sub == sq
            inv = 1.0 / pivot
            scale[gq] = jnp.where(here, inv, scale[gq])
            if q + 1 < step:
                gn, sn = (q + 1) // 8, (q + 1) % 8
                product = row(c[q][gn], sn) * row(c[q + 1][gq], sq)
                pivot = row(c[q + 1][gn], sn) - product * inv
            factor = [jnp.where(here, 0.0, c[q][i]) if i == gq else c[q][i] for i in range(per)]
            factor = [f * inv for f in factor]
            for p in range(q + 1, step):
                pivot_row = row(c[p][gq], sq)
                for i in range(per):
                    c[p][i] = c[p][i] - factor[i] * pivot_row
            for w in range(wide):
                pivot_row = row(panel[gq][w], sq)
                for i in range(per):
                    panel[i][w] = panel[i][w] - factor[i] * pivot_row
        done = [[panel[i][w] * scale[i] for w in range(wide)] for i in range(per)]
        lanes = lax.broadcasted_iota(jnp.int32, (step, size), 1)
        left = stack(now)
        left = thirds(jnp.where(lanes < first, -left, left))
        right = thirds(stack(done))
        update = lax.dot_general(
            jnp.concatenate([left[i] for i, _ in pairs], axis=0),
            jnp.concatenate([right[i] for _, i in pairs], axis=0),
            (((0,), (0,)), ((), ())),
            preferred_element_type=jnp.float32,
        )
        if more:
            now = []
            for i in range(per):
                fresh = []
                for w in range(wide):
                    terms = [ahead_c[q][i] * row(done[q // 8][w], q % 8) for q in range(step)]
                    while len(terms) > 1:
                        terms = [x + y for x, y in zip(terms[::2], terms[1::2])]
                    spread = terms[0]
                    base = ahead[i][w]
                    base = jnp.where(inside, 0.0, base) if w == w0 else base
                    fresh.append(base - spread)
                now.append(fresh)
        for g in range(size // 8):
            for w in range(wide):
                if g0 <= g < g0 + per:
                    value = done[g - g0][w]
                elif more and g0 + per <= g < g0 + 2 * per:
                    value = now[g - g0 - per][w]
                else:
                    value = tile(g, w)
                    value = jnp.where(inside, 0.0, value) if w == w0 else value
                    value = value - update[8 * g : 8 * g + 8, 128 * w : 128 * w + 128]
                a[8 * g : 8 * g + 8, 128 * w : 128 * w + 128] = value


def first_kernel(nj, nk, height_b, flipped, blocks, held, c_cols, b_cols, *refs):
    where = place()
    owns, (away, out, b_all) = refs[:nk], refs[nk:]
    rank = out.shape[1]
    pieces = []
    for t in range(1, nk):
        pieces += contraction(held.at[t, : nj // 2], away.at[t - 1], c_cols[...], b_cols[...])
    turns = blocks // 16 + 1

    def gram(x, contracted):
        dims = (((contracted,), (contracted,)), ((), ()))
        return lax.dot_general(x, x, dims, preferred_element_type=jnp.float32)

    for t in range(nk):
        part = owns[t][rank:, :].reshape(nj, height_b, owns[t].shape[1])
        if flipped:
            at = pl.multiple_of(wrap(where[1] - t, nk) * height_b, height_b)
            b_all[:, pl.ds(at, height_b), :] = part
        else:
            at = pl.multiple_of(wrap(where[1] - t, nk) * 128, 128)
            b_all[:, :, pl.ds(at, 128)] = part
    if flipped:
        gram_b = sum(gram(b_all[s], 1) for s in range(nj))
    else:
        gram_b = gram(b_all[...].reshape(nj * height_b, rank), 0)
    gram_c = sum(gram(own[:rank, :], 1) for own in owns)
    share(pieces, 0, turns)
    diagonal = lax.broadcasted_iota(jnp.int32, out.shape, 0) == lax.broadcasted_iota(
        jnp.int32, out.shape, 1
    )
    out[...] = gram_b * gram_c + jnp.where(diagonal, ridge_weight, 0.0)
    invert(out, 0, blocks, lambda turn: share(pieces, turn + 1, turns))


def middle_kernel(begin, end, held, c_cols, b_cols, started, kept, out):
    out[...] = started[...]
    half = kept.shape[0]
    pieces = contraction(held.at[0, :half], kept, c_cols[...], b_cols[...])
    turns = (end - begin) // 16
    invert(out, begin, end, lambda turn: share(pieces, turn, turns))


def rest_kernel(blocks, half_done, out):
    out[...] = half_done[...]
    invert(out, blocks, out.shape[0])


def solve_kernel(kept, received, inverse, out):
    left, right = thirds(kept[0] + received[0]), thirds(inverse[...])
    out[...] = jnp.dot(
        jnp.concatenate([left[i] for i, _ in pairs], axis=1),
        jnp.concatenate([right[i] for _, i in pairs], axis=0),
        preferred_element_type=jnp.float32,
    )


def send(x, axis, n, s):
    return lax.ppermute(x, axis, shift(n, s))


def update(tensor, factor_b, factor_c):
    nj, nk = lax.axis_size("ja"), lax.axis_size("ka")
    rank = factor_b.shape[1] * nk
    flipped = factor_b.shape[1] % 128 != 0
    part_b = factor_b.T if flipped else factor_b
    height_b = part_b.shape[0]
    mine = jnp.concatenate([part_b, factor_c.T], axis=0)
    line = [mine] + [send(mine, "ja", nj, s) for s in range(1, nj)]
    b_parts = [mine] + [send(mine, "ka", nk, t) for t in range(1, nk)]
    held = fetch(tensor, nj, nk)
    away, own, c_cols, b_cols = contract_away(
        held, line, b_parts, height_b, flipped, rank
    )
    half = nj // 2
    turns = tuple(range(1, nk))
    owns = [own] + [send(own, "ka", nk, t) for t in turns]
    sent = contract_rows((0,), half, half, held, c_cols, b_cols)[0]
    for t in turns:
        sent = sent + send(away[t - 1], "ka", nk, t)
    received = lax.ppermute(sent, "ja", [(i, i ^ 1) for i in range(nj)])
    params = pltpu.CompilerParams(vmem_limit_bytes=20 * 2**20)
    cost = pl.CostEstimate(flops=5 * 10**9, bytes_accessed=2**20, transcendentals=0)
    square = jax.ShapeDtypeStruct((rank, rank), jnp.float32)
    first, middle = rank // 128 * 16, rank // 256 * 96
    b_shape = (nj, rank, mine.shape[1]) if flipped else (nj, height_b, rank)
    away, started = pl.pallas_call(
        functools.partial(first_kernel, nj, nk, height_b, flipped, first),
        out_shape=[jax.ShapeDtypeStruct(away.shape, jnp.float32), square],
        in_specs=[vmem] * (3 + nk),
        out_specs=[vmem] * 2,
        scratch_shapes=[pltpu.VMEM(b_shape, mine.dtype)],
        compiler_params=params,
        cost_estimate=cost,
    )(held, c_cols, b_cols, *owns)
    kept, half_done = pl.pallas_call(
        functools.partial(middle_kernel, first, middle),
        out_shape=[jax.ShapeDtypeStruct(sent.shape, jnp.float32), square],
        in_specs=[vmem] * 4,
        out_specs=[vmem] * 2,
        compiler_params=params,
        cost_estimate=cost,
    )(held, c_cols, b_cols, started)
    for t in turns:
        kept = kept + send(away[t - 1], "ka", nk, t)
    bit = 2
    while bit < nj:
        kept, sent = jnp.split(kept + received, 2, axis=0)
        received = lax.ppermute(sent, "ja", [(i, i ^ bit) for i in range(nj)])
        bit *= 2
    inverse = pl.pallas_call(
        functools.partial(rest_kernel, middle),
        out_shape=square,
        in_specs=[vmem],
        out_specs=vmem,
        compiler_params=params,
        cost_estimate=cost,
    )(half_done)
    return pl.pallas_call(
        solve_kernel,
        out_shape=jax.ShapeDtypeStruct(kept.shape[1:], jnp.float32),
        in_specs=[vmem] * 3,
        out_specs=vmem,
        compiler_params=params,
        cost_estimate=pl.CostEstimate(flops=10**8, bytes_accessed=2**19, transcendentals=0),
    )(kept, received, inverse)


def solution(mesh):
    placed = (P("ia", "ja", "ka"), P("ja", "ka"), P("ka", "ja"))
    return jax.shard_map(
        update, mesh=mesh, in_specs=placed, out_specs=P(("ia", "ja", "ka"), None), check_vma=False
    )
```
